32 devices in a mesh: section: 8 (over y, x, core), tp: 4 (over z).
Axes of the slice: x: 2, y: 2, z: 4, core: 2. Of those that a mesh axis runs over, the one named last changes fastest.
Arguments:
- stash: bfloat16 [8, 2, 256, 4096], P('section', None, 'tp'), may hold values from -660 to 660
- slot: int32 [8], P('section'), may hold values from 0 to 1
- doc_ids: int32 [8, 2, 256], P('section', None, 'tp'), may hold values from 0 to 3, never falling along the last dimension, each value on 1 to 128 neighbouring positions
- norm_gain: bfloat16 [4096], replicated, may hold values from 0.099609375 to 1.8984375
- w_query: bfloat16 [4096, 4096], P(None, 'tp'), may hold values from -21 to 21
- w_key: bfloat16 [4096, 1024], P(None, 'tp'), may hold values from -21 to 21
- value_weight: bfloat16 [4096, 1024], P(None, 'tp'), may hold values from -0.09375 to 0.09375
Outputs:
- received: bfloat16 [8, 256, 4096], P('section', None, 'tp')
The draws below stay inside these ranges and needn't reach their ends.
Inputs may be any that keep to these rules, and one draw needn't show every extreme that they name: `doc_ids`: document numbers never fall along a micro-batch.
All inputs are finite; a program needn't handle non-finite values.
Results may differ from the reference program's by a relative error of at most 0.025.
The reference program's roundings to bfloat16 on the way (of `picked`, `normed`, `values`, `softmax_weights` and `context`) count: a program that leaves them out, or rounds other values in their place, can miss the bound.
Values may be sent and summed in bfloat16 or wider, within the bound.
A program may use at most 64 MiB of HBM per device.

```python
import math
import jax
import jax.numpy as jnp
import numpy as np
from jax import lax

MODEL_WIDTH = 4096
HQ = 32
VALUE_KEY_HEADS = 8
HEAD_SIZE = 128
SLOTS = 2
DOCS = 4
TOK = 256
SECTIONS = 8


def weight_with_spike(key, salt_value, columns):
    gaussian = jax.random.truncated_normal(jax.random.fold_in(key, salt_value), -4.0, 4.0, (MODEL_WIDTH, columns), jnp.float32)
    gaussian = gaussian / jnp.sqrt(jnp.float32(MODEL_WIDTH))
    return gaussian.astype(jnp.bfloat16)


def draw_w_query(key, part):
    return weight_with_spike(key, 1, HQ * HEAD_SIZE)


def draw_w_key(key, part):
    return weight_with_spike(key, 2, VALUE_KEY_HEADS * HEAD_SIZE)


def draw_stash(key, part):
    full_shape = (SECTIONS, SLOTS, TOK, MODEL_WIDTH)
    col_scale = jnp.exp(jax.random.uniform(jax.random.fold_in(key, 12), (MODEL_WIDTH,), jnp.float32, 0.0, math.log(10.0)))
    row_scale = jnp.exp(jax.random.uniform(jax.random.fold_in(key, 11), (SECTIONS, SLOTS, TOK, 1), jnp.float32, 0.0, math.log(10.0)))
    noise_part = jax.random.truncated_normal(jax.random.fold_in(key, 13), -4.0, 4.0, full_shape, jnp.float32)
    result = noise_part * row_scale * col_scale
    return result.astype(jnp.bfloat16)


def place_ends(values, rng, low, largest):
    dims = values.shape
    spot = [jax.random.randint(jax.random.fold_in(rng, axis), (), 0, dims[axis]) for axis in range(len(dims))]
    values = values.at[tuple(spot)].set(low)
    longest = dims.index(max(dims))
    spot[longest] = (spot[longest] + 1) % dims[longest]
    return values.at[tuple(spot)].set(largest)


def block_levels(key, extent, cuts, least, largest):
    level, own = 1.0, jax.random.fold_in(key, 6)
    for position, shards_of in cuts:
        steps = jnp.exp(jax.random.uniform(jax.random.fold_in(own, position), (shards_of,), jnp.float32, least / len(cuts), largest / len(cuts)))
        level = level * jnp.repeat(steps, extent[position] // shards_of).reshape([-1 if axis == position else 1 for axis in range(len(extent))])
    return level


def length_profile(amount, total, bound, slope):
    loads = [(1 << 20) // math.isqrt(grade ** slope) + 1 for grade in range(2, amount + 1)]
    rest, holding = total - bound - (amount - 1), [1] * (amount - 1)
    while rest > 0:
        movable = [i for i in range(amount - 1) if holding[i] < bound]
        mass, remaining = sum([loads[i] for i in movable]), rest
        for i in movable:
            extra = min(bound - holding[i], max(1, remaining * loads[i] // mass), rest)
            holding[i] = holding[i] + extra
            rest = rest - extra
    return np.array([bound] + holding)


def ragged(key, count, total, most, lean):
    if count == 2:
        one = jax.random.randint(key, (), max(1, total - most), min(most, total - 1) + 1)
        return jnp.stack([one, total - one])
    tallies = jnp.asarray(length_profile(count, total, most, lean), jnp.int32)
    pairs = (count - 1) // 2
    donor, receiver = tallies[1:1 + 2 * pairs:2], tallies[2:2 + 2 * pairs:2]
    slack = jnp.minimum(donor - 1, most - receiver)
    moved = jax.random.randint(jax.random.fold_in(key, 1), (pairs,), 0, 1 << 20) % (slack + 1)
    tallies = tallies.at[1:1 + 2 * pairs:2].set(donor - moved).at[2:2 + 2 * pairs:2].set(receiver + moved)
    return tallies[jax.random.permutation(jax.random.fold_in(key, 2), count)]


def noise(stream_key, extent, width, most, split=(), kind=jnp.bfloat16):
    entries = jax.random.normal(stream_key, extent, jnp.float32) * width
    if len(split) > 0:
        entries = block_levels(stream_key, extent, split, -0.22, 0.18) * entries
    return jnp.clip(entries, min=-most, max=most).astype(kind)


def setup_inputs(seed: int = 0) -> dict:
    splits = jax.random.split(jax.random.key(seed), 8)
    stash = draw_stash(jax.random.fold_in(splits[7], 71), 0)
    slot = place_ends(jax.random.randint(splits[1], (SECTIONS,), 0, SLOTS), jax.random.fold_in(splits[1], 1), 0, SLOTS - 1).astype(jnp.int32)
    doc_ids = jax.vmap(lambda own: jnp.searchsorted(jnp.cumsum(ragged(own, DOCS, TOK, TOK // 2, 1)), jnp.arange(TOK), side="right"))(jax.random.split(splits[2], SECTIONS * SLOTS)).reshape((SECTIONS, SLOTS, TOK)).astype(jnp.int32)
    norm_gain = jnp.clip(1.0 + 0.18 * jax.random.normal(splits[3], (MODEL_WIDTH,), jnp.float32), 0.099609375, 1.8984375).astype(jnp.bfloat16)
    w_query = draw_w_query(jax.random.fold_in(splits[7], 71), 0)
    w_key = draw_w_key(jax.random.fold_in(splits[7], 71), 0)
    value_weight = noise(splits[6], (MODEL_WIDTH, VALUE_KEY_HEADS * HEAD_SIZE), MODEL_WIDTH ** -0.5, 0.09375, ((1, 4),))
    return dict(stash=stash, slot=slot, doc_ids=doc_ids, norm_gain=norm_gain, w_query=w_query, w_key=w_key, value_weight=value_weight)


ROPE_BASE = 500000.0
NORM_EPSILON = 1e-05

def rotate(values, positions):
    head_width = values.shape[-1]
    half_width = head_width // 2
    freq_index = jnp.arange(half_width, dtype=jnp.float32)
    inverse = jnp.power(jnp.float32(ROPE_BASE), -2.0 * freq_index / head_width)
    angles = positions.astype(jnp.float32)[:, None] * inverse[None, :]
    cosine = jnp.concatenate([jnp.cos(angles), jnp.cos(angles)], -1)[:, None, :]
    sine_part = jnp.concatenate([jnp.sin(angles), jnp.sin(angles)], -1)[:, None, :]
    turned = jnp.concatenate([-values[..., half_width:], values[..., :half_width]], -1)
    return values * cosine + turned * sine_part

def normalize(stash_rows, norm_gain):
    widened = stash_rows.astype(jnp.float32)
    mean_square = lax.optimization_barrier(jnp.mean(widened * widened, axis=-1, keepdims=True))
    return (widened * lax.rsqrt(mean_square + NORM_EPSILON) * norm_gain.astype(jnp.float32)).astype(jnp.bfloat16)

def project(normed, weight, positions, use_rope):
    length = normed.shape[0]
    product = jnp.dot(normed, weight, preferred_element_type=jnp.float32)
    if use_rope:
        product = rotate(product.reshape(length, -1, HEAD_SIZE), positions).reshape(length, -1)
    return product.astype(jnp.bfloat16)

def attend(queries, keys, values, doc_rows):
    length = queries.shape[0]
    kv_count = keys.shape[1] // HEAD_SIZE
    group_size = queries.shape[1] // HEAD_SIZE // kv_count
    grouped = queries.astype(jnp.float32).reshape(length, kv_count, group_size, HEAD_SIZE)
    key_heads = keys.astype(jnp.float32).reshape(length, kv_count, HEAD_SIZE)
    value_heads = values.astype(jnp.float32).reshape(length, kv_count, HEAD_SIZE)
    scores = jnp.einsum('ihgd,jhd->hgij', grouped, key_heads) * (1.0 / math.sqrt(HEAD_SIZE))
    row_index = jnp.arange(length, dtype=jnp.int32)[:, None]
    col_index = jnp.arange(length, dtype=jnp.int32)[None, :]
    allowed = (col_index <= row_index) & (doc_rows[None, :] == doc_rows[:, None])
    scores = jnp.where(allowed, scores, -1e+30)
    row_max = lax.optimization_barrier(jnp.max(scores, axis=-1, keepdims=True))
    score_exponent = jnp.exp(scores - row_max)
    softmax_weights = (score_exponent / lax.optimization_barrier(jnp.sum(score_exponent, axis=-1, keepdims=True))).astype(jnp.bfloat16)
    context = jnp.einsum('hgij,jhd->ihgd', softmax_weights.astype(jnp.float32), value_heads)
    return context.reshape(length, -1).astype(jnp.bfloat16)

def reference(stash, slot, doc_ids, norm_gain, w_query, w_key, value_weight):
    positions = jnp.arange(TOK, dtype=jnp.int32)

    def one_section(inputs):
        section_stash, section_slot, section_docs = inputs
        picked = lax.dynamic_index_in_dim(section_stash, section_slot, 0, keepdims=False)
        doc_rows = lax.dynamic_index_in_dim(section_docs, section_slot, 0, keepdims=False)
        normed = normalize(picked, norm_gain)
        queries = project(normed, w_query, positions, True)
        keys = project(normed, w_key, positions, True)
        values = project(normed, value_weight, positions, False)
        return attend(queries, keys, values, doc_rows)
    context_rows = lax.map(one_section, (stash, slot, doc_ids))
    return jnp.concatenate([jnp.zeros_like(context_rows[:1]), context_rows[:-1]], 0)
```

```python
import functools
import math

import jax
import jax.numpy as jnp
import numpy as np
from jax import lax
from jax.experimental import pallas as pl
from jax.experimental.pallas import tpu as pltpu
from jax.sharding import PartitionSpec as P

HEAD_SIZE = 128
ROPE_BASE = 500000.0
NORM_EPSILON = 1e-05
PIECES = 4
MESH = pl.DeviceIdType.MESH
GATHER_VMEM = 26 << 20
ATTEND_VMEM = 8 << 20
ANY = pl.BlockSpec(memory_space=pltpu.HBM)
VMEM = pl.BlockSpec(memory_space=pltpu.VMEM)


def rope_tables(length):
    half = HEAD_SIZE // 2
    freq = np.arange(half, dtype=np.float32)
    inverse = np.power(np.float32(ROPE_BASE), np.float32(-2.0) * freq / np.float32(HEAD_SIZE)).astype(np.float32)
    angles = np.arange(length, dtype=np.float32)[:, None] * inverse[None, :]
    cos, sin = np.cos(angles), np.sin(angles)
    return (
        np.concatenate([cos, cos], -1).astype(np.float32),
        np.concatenate([-sin, sin], -1).astype(np.float32),
    )


def early_pieces(sec, ns):
    pairs = ns // 2
    count = PIECES * jnp.maximum(pairs - 1 - sec // 2, 0) // pairs if pairs else 0 * sec
    first = jnp.where((sec > 0) & (sec + 2 == ns), 1, 0)
    return jnp.where((sec % 2 == 1) & (sec + 1 < ns), count, first)


def kernel(
    n, ns,
    slot_ref, stash_ref, doc_hbm, gain_hbm, cos_hbm, sin_hbm, wq_ref, wk_ref, wv_ref,
    q, k, v, dcol, drow,
    raw, mine, dmine, w, xbuf, zbuf, dbuf, acc,
    raw_sem, w_sem, shift_send, left_send, recv,
    zleft_send, zrecv,
    dshift_send, dleft_send, drecv,
    doc_ref, gain_ref, cos_ref, sin_ref, small_sem,
):
    me = lax.axis_index("tp")
    sec = lax.axis_index("section")
    slots, rows, width = raw.shape
    pieces = PIECES
    part = width // pieces
    nq, nk = wq_ref.shape[1], wk_ref.shape[1]
    total_n = w.shape[2]
    total = n * rows
    has_right, has_left = me + 1 < n, me > 0
    has_next, has_prev = sec + 1 < ns, sec > 0
    early, early_prev = early_pieces(sec, ns), early_pieces(sec - 1, ns)

    raw_copy = pltpu.make_async_copy(stash_ref.at[0], raw, raw_sem)
    raw_copy.start()
    small = [
        pltpu.make_async_copy(src, dst, small_sem.at[i])
        for i, (src, dst) in enumerate(
            ((gain_hbm, gain_ref), (doc_hbm, doc_ref), (cos_hbm, cos_ref), (sin_hbm, sin_ref))
        )
    ]
    for c in small:
        c.start()

    bar = pltpu.get_barrier_semaphore()
    for cond, target in (
        (has_right, {"tp": me + 1}),
        (has_left, {"tp": me - 1}),
        (has_next, {"section": sec + 1}),
        (has_prev, {"section": sec - 1}),
    ):
        @pl.when(cond)
        def _():
            pl.semaphore_signal(bar, inc=1, device_id=target, device_id_type=MESH)

    def w_copies(p):
        span = pl.ds(pl.multiple_of(p * part, part), part)
        return (
            pltpu.make_async_copy(wq_ref.at[span], w.at[p, :, 0:nq], w_sem.at[p]),
            pltpu.make_async_copy(wk_ref.at[span], w.at[p, :, nq:nq + nk], w_sem.at[p]),
            pltpu.make_async_copy(wv_ref.at[span], w.at[p, :, nq + nk:total_n], w_sem.at[p]),
        )

    def w_wait(p):
        pltpu.make_async_copy(w.at[p], w.at[p], w_sem.at[p]).wait()

    chosen = slot_ref[0]
    dmine[...] = jnp.zeros_like(dmine)
    for c in small:
        c.wait()
    docs = doc_ref[0, 0:1, :]
    for i in range(1, slots):
        docs = jnp.where(jnp.full(docs.shape, chosen, jnp.int32) == i, doc_ref[0, i:i + 1, :], docs)
    dmine[0:1, 0:rows] = docs
    raw_copy.wait()

    @pl.when(has_prev)
    def _():
        for p in range(pieces):
            for c in w_copies(p):
                c.start()

    step = 16
    for r in range(0, rows, step):
        x = raw[0, r:r + step, :]
        for i in range(1, slots):
            x = jnp.where(jnp.full(x.shape, chosen, jnp.int32) == i, raw[i, r:r + step, :], x)
        x = x.astype(jnp.float32)
        scale = lax.rsqrt(jnp.mean(x * x, axis=-1, keepdims=True) + NORM_EPSILON)
        y = (x * scale * gain_ref[...].astype(jnp.float32)[None, :]).astype(jnp.bfloat16)
        for p in range(pieces):
            mine[p, r:r + step, :] = y[:, p * part:(p + 1) * part]

    def edges(a):
        return a.astype(jnp.int32)

    pl.semaphore_wait(bar, edges(has_right) + edges(has_left) + edges(has_next) + edges(has_prev))

    def remote(src, dst, ss, rs, target):
        return pltpu.make_async_remote_copy(
            src_ref=src, dst_ref=dst, send_sem=ss, recv_sem=rs, device_id=target, device_id_type=MESH
        )

    def hop(src, c, p):
        return remote(src, xbuf.at[c, p], shift_send.at[c, p], recv.at[c, p], {"section": sec + 1})

    def shift(p):
        return hop(mine.at[p], me, p)

    def zright(src, c, p):
        return remote(src, zbuf.at[c, p], zrecv.at[c, p], zrecv.at[c, p], {"tp": me + 1})

    def zleft(src, c, p, own=False):
        ss = zleft_send.at[p] if own else zrecv.at[c, p]
        return remote(src, zbuf.at[c, p], ss, zrecv.at[c, p], {"tp": me - 1})

    def dshift():
        return remote(dmine, dbuf.at[me], dshift_send, drecv.at[me], {"section": sec + 1})

    def right(c, p):
        b = xbuf.at[c, p]
        return remote(b, b, recv.at[c, p], recv.at[c, p], {"tp": me + 1})

    def left(c, p, own=False):
        b = xbuf.at[c, p]
        ss = left_send.at[p] if own else recv.at[c, p]
        return remote(b, b, ss, recv.at[c, p], {"tp": me - 1})

    def dright(c):
        b = dbuf.at[c]
        return remote(b, b, drecv.at[c], drecv.at[c], {"tp": me + 1})

    def dleft(c, own=False):
        b = dbuf.at[c]
        return remote(b, b, dleft_send if own else drecv.at[c], drecv.at[c], {"tp": me - 1})

    @pl.when(has_next)
    def _():
        dshift().start()
        for p in range(pieces):
            shift(p).start()

            @pl.when(has_right & (p < early))
            def _():
                zright(mine.at[p], me, p).start()

            @pl.when(has_left & (p < early))
            def _():
                zleft(mine.at[p], me, p, True).start()

    tile = 256

    def compute(c, p, last):
        x = xbuf[c, p]
        for t in range(0, total_n, tile):
            acc[c, :, t:t + tile] += jnp.dot(x, w[p, :, t:t + tile], preferred_element_type=jnp.float32)

        if last is False:
            return

        @pl.when(last)
        def _():
            span = pl.ds(pl.multiple_of(c * rows, rows), rows)
            cos, sin = cos_ref[span, :], sin_ref[span, :]
            for h in range(0, nq + nk, HEAD_SIZE):
                u = acc[c, :, h:h + HEAD_SIZE]
                u = (u * cos + pltpu.roll(u, HEAD_SIZE // 2, 1) * sin).astype(jnp.bfloat16)
                if h < nq:
                    q[span, h:h + HEAD_SIZE] = u
                else:
                    k[span, h - nq:h - nq + HEAD_SIZE] = u
            v[span, :] = acc[c, :, nq + nk:total_n].astype(jnp.bfloat16)

    def own_forward(p):
        @pl.when(has_right & (p >= early_prev))
        def _():
            right(me, p).start()

        @pl.when(has_left & (p >= early_prev))
        def _():
            left(me, p, True).start()

    def keep_docs(c):
        drow[c] = dbuf[c]
        lanes = dbuf.shape[2]
        wide = jnp.broadcast_to(dbuf[c, 0:1, :].astype(jnp.float32), (lanes, lanes))
        dcol[pl.ds(pl.multiple_of(c * rows, rows), rows), :] = wide.T[0:rows, :]

    @pl.when(has_prev)
    def _():
        acc[...] = jnp.zeros_like(acc)
        dshift().wait_recv()

        @pl.when(has_right)
        def _():
            dright(me).start()

        @pl.when(has_left)
        def _():
            dleft(me, True).start()

        keep_docs(me)

        @pl.loop(0, pieces)
        def _(p):
            shift(p).wait_recv()
            own_forward(p)

        @pl.loop(0, pieces)
        def _(p):
            w_wait(p)
            compute(me, p, p == pieces - 1)

    def pass_early(d, p):
        below, above = me - d, me + d

        @pl.when(below >= 0)
        def _():
            b = zbuf.at[below, p]
            zright(b, below, p).wait_recv()

            @pl.when(has_right)
            def _():
                zright(b, below, p).start()

            hop(b, below, p).start()

        @pl.when(above < n)
        def _():
            b = zbuf.at[above, p]
            zleft(b, above, p).wait_recv()

            @pl.when(has_left)
            def _():
                zleft(b, above, p).start()

            hop(b, above, p).start()

    def take_early(below, above):
        @pl.loop(0, 2 * pieces)
        def _(i):
            c = jnp.where(i < pieces, below, above)
            p = i % pieces

            @pl.when((c >= 0) & (c < n) & (p < early_prev))
            def _():
                hop(xbuf.at[c, p], c, p).wait_recv()
                compute(c, p, False)

    @pl.when(has_prev)
    def _():
        @pl.loop(0, (n - 1) * pieces)
        def _(i):
            d, p = i // pieces + 1, i % pieces
            below, above = me - d, me + d
            late = p >= early_prev

            @pl.when(p == 0)
            def _():
                @pl.loop(0, pieces)
                def _(e):
                    @pl.when(e < early)
                    def _():
                        pass_early(d, e)

            @pl.when((below >= 0) & (p == 0))
            def _():
                dright(below).wait_recv()

                @pl.when(has_right)
                def _():
                    dright(below).start()

                keep_docs(below)

            @pl.when((above < n) & (p == 0))
            def _():
                dleft(above).wait_recv()

                @pl.when(has_left)
                def _():
                    dleft(above).start()

                keep_docs(above)

            final = p == pieces - 1

            @pl.when(final & (d == n - 1))
            def _():
                take_early(below, above)

            @pl.when(late & (below >= 0))
            def _():
                right(below, p).wait_recv()

                @pl.when(has_right)
                def _():
                    right(below, p).start()

            @pl.when(late & (above < n))
            def _():
                left(above, p).wait_recv()

                @pl.when(has_left)
                def _():
                    left(above, p).start()

            @pl.when(final & (d < n - 1))
            def _():
                take_early(below, above)

            @pl.when(late & (below >= 0))
            def _():
                compute(below, p, final)

            @pl.when(late & (above < n))
            def _():
                compute(above, p, final)

        @pl.when(has_right)
        def _():
            dright(me).wait_send()

        @pl.when(has_left)
        def _():
            dleft(me, True).wait_send()

        for p in range(pieces):
            @pl.when(has_right & (p >= early_prev))
            def _():
                right(me, p).wait_send()

            @pl.when(has_left & (p >= early_prev))
            def _():
                left(me, p, True).wait_send()

        for d in range(1, n):
            below, above = me - d, me + d

            @pl.when((below >= 0) & has_right)
            def _():
                dright(below).wait_send()
                for p in range(pieces):
                    @pl.when(p >= early_prev)
                    def _():
                        right(below, p).wait_send()

            @pl.when((above < n) & has_left)
            def _():
                dleft(above).wait_send()
                for p in range(pieces):
                    @pl.when(p >= early_prev)
                    def _():
                        left(above, p).wait_send()

    @pl.when(has_next)
    def _():
        dshift().wait_send()
        for p in range(pieces):
            shift(p).wait_send()

            @pl.when(has_right & (p < early))
            def _():
                zright(mine.at[p], me, p).wait_send()

            @pl.when(has_left & (p < early))
            def _():
                zleft(mine.at[p], me, p, True).wait_send()

        for d in range(1, n):
            below, above = me - d, me + d

            @pl.when((below >= 0) & (early > 0))
            def _():
                for p in range(pieces):
                    @pl.when(p < early)
                    def _():
                        hop(zbuf.at[below, p], below, p).wait_send()

                    @pl.when(has_right & (p < early))
                    def _():
                        zright(zbuf.at[below, p], below, p).wait_send()

            @pl.when((above < n) & (early > 0))
            def _():
                for p in range(pieces):
                    @pl.when(p < early)
                    def _():
                        hop(zbuf.at[above, p], above, p).wait_send()

                    @pl.when(has_left & (p < early))
                    def _():
                        zleft(zbuf.at[above, p], above, p).wait_send()


def attend(n, rows, q, k, v, dcol, drow, out_ref, s_buf, p_buf):
    sec = lax.axis_index("section")
    g = pl.program_id(0)
    total = n * rows
    group = out_ref.shape[2] // HEAD_SIZE
    block = 128 if total % 128 == 0 else total
    factor = math.log2(math.e) / math.sqrt(HEAD_SIZE)

    @pl.when(sec == 0)
    def _():
        out_ref[...] = jnp.zeros_like(out_ref)

    @pl.when(sec > 0)
    def _():
        lane_docs = jnp.concatenate([drow[c, 0:1, 0:rows] for c in range(n)], axis=1).astype(jnp.float32)
        cols = pl.ds(pl.multiple_of(g * HEAD_SIZE, HEAD_SIZE), HEAD_SIZE)
        vg = v[:, cols]
        vg = jnp.concatenate([vg, jnp.ones_like(vg)], axis=1)
        starts = range(0, total, block)
        for i in starts:
            upto = i + block
            keys = k[0:upto, cols]
            i_idx = lax.broadcasted_iota(jnp.int32, (block, upto), 0) + i
            j_idx = lax.broadcasted_iota(jnp.int32, (block, upto), 1)
            allowed = (j_idx <= i_idx) & (dcol[i:upto, 0:1] == lane_docs[:, 0:upto])
            for h in range(group):
                wide = pl.ds(pl.multiple_of((g * group + h) * HEAD_SIZE, HEAD_SIZE), HEAD_SIZE)
                raw = lax.dot_general(
                    q[i:upto, wide], keys, (((1,), (1,)), ((), ())), preferred_element_type=jnp.float32
                )
                s_buf[h, i:upto, 0:upto] = jnp.where(allowed, raw, -1e30)
        for i in starts:
            upto = i + block
            for h in range(group):
                x = s_buf[h, i:upto, 0:upto]
                e = jnp.exp2((x - jnp.max(x, axis=-1, keepdims=True)) * factor)
                p_buf[h, i:upto, 0:upto] = e.astype(jnp.bfloat16)
        for i in starts:
            upto = i + block
            for h in range(group):
                both = jnp.dot(p_buf[h, i:upto, 0:upto], vg[0:upto], preferred_element_type=jnp.float32)
                out_ref[0, i:upto, h * HEAD_SIZE:(h + 1) * HEAD_SIZE] = (
                    both[:, 0:HEAD_SIZE] / both[:, HEAD_SIZE:]
                ).astype(jnp.bfloat16)


def in_hbm(a):
    return pltpu.with_memory_space_constraint(a, pltpu.HBM)


def per_device(stash, slot, doc_ids, norm_gain, w_query, w_key, value_weight):
    stash, doc_ids, norm_gain, w_query, w_key, value_weight = (
        in_hbm(a) for a in (stash, doc_ids, norm_gain, w_query, w_key, value_weight)
    )
    n, ns = lax.axis_size("tp"), lax.axis_size("section")
    _, slots, rows, width = stash.shape
    total = n * rows
    nq, nk = w_query.shape[1], w_key.shape[1]
    total_n = nq + nk + value_weight.shape[1]
    cos, sin = (in_hbm(jnp.asarray(t)) for t in rope_tables(total))
    lanes = -(-rows // 128) * 128
    bf, f32, dma = jnp.bfloat16, jnp.float32, pltpu.SemaphoreType.DMA
    part = width // PIECES
    q, k, v, dcol, drow = pl.pallas_call(
        functools.partial(kernel, n, ns),
        out_shape=(
            jax.ShapeDtypeStruct((total, nq), bf),
            jax.ShapeDtypeStruct((total, nk), bf),
            jax.ShapeDtypeStruct((total, nk), bf),
            jax.ShapeDtypeStruct((total, lanes), f32),
            jax.ShapeDtypeStruct((n, 8, lanes), jnp.int32),
        ),
        in_specs=[pl.BlockSpec(memory_space=pltpu.SMEM)] + [ANY] * 8,
        out_specs=(VMEM,) * 5,
        scratch_shapes=[
            pltpu.VMEM((slots, rows, width), bf),
            pltpu.VMEM((PIECES, rows, part), bf),
            pltpu.VMEM((8, lanes), jnp.int32),
            pltpu.VMEM((PIECES, part, total_n), bf),
            pltpu.VMEM((n, PIECES, rows, part), bf),
            pltpu.VMEM((n, PIECES, rows, part), bf),
            pltpu.VMEM((n, 8, lanes), jnp.int32),
            pltpu.VMEM((n, rows, total_n), f32),
            dma,
            dma((PIECES,)),
            dma((n, PIECES)),
            dma((PIECES,)),
            dma((n, PIECES)),
            dma((PIECES,)),
            dma((n, PIECES)),
            dma,
            dma,
            dma((n,)),
            pltpu.VMEM(doc_ids.shape, jnp.int32),
            pltpu.VMEM(norm_gain.shape, bf),
            pltpu.VMEM(cos.shape, f32),
            pltpu.VMEM(sin.shape, f32),
            dma((4,)),
        ],
        compiler_params=pltpu.CompilerParams(
            collective_id=0, has_side_effects=True, vmem_limit_bytes=GATHER_VMEM
        ),
        cost_estimate=pl.CostEstimate(
            flops=2 * total * width * total_n, bytes_accessed=width * total_n * 2, transcendentals=0
        ),
    )(slot, stash, doc_ids, norm_gain, cos, sin, w_query, w_key, value_weight)
    heads = nk // HEAD_SIZE
    return pl.pallas_call(
        functools.partial(attend, n, rows),
        grid=(heads,),
        out_shape=jax.ShapeDtypeStruct((1, total, nq), bf),
        in_specs=[VMEM] * 5,
        out_specs=pl.BlockSpec((1, total, nq // heads), lambda g: (0, 0, g)),
        scratch_shapes=[
            pltpu.VMEM((nq // nk, total, total), f32),
            pltpu.VMEM((nq // nk, total, total), bf),
        ],
        compiler_params=pltpu.CompilerParams(vmem_limit_bytes=ATTEND_VMEM),
    )(q, k, v, dcol, drow)


def solution(mesh):
    placed = (
        P("section", None, "tp", None),
        P("section"),
        P("section", None, "tp"),
        P(),
        P(None, "tp"),
        P(None, "tp"),
        P(None, "tp"),
    )
    return jax.shard_map(
        per_device, mesh=mesh, in_specs=placed, out_specs=P("section", None, "tp"), check_vma=False
    )
```

```python
import functools
import math

import jax
import jax.numpy as jnp
import numpy as np
from jax import lax
from jax.experimental import pallas as pl
from jax.experimental.pallas import tpu as pltpu
from jax.sharding import PartitionSpec as P

HEAD_SIZE = 128
ROPE_BASE = 500000.0
NORM_EPSILON = 1e-05
PIECES = 4
HELD = 1
CHUNK = 16
MESH = pl.DeviceIdType.MESH
VMEM_GRANT = 32 << 20
ANY = pl.BlockSpec(memory_space=pltpu.HBM)
VMEM = pl.BlockSpec(memory_space=pltpu.VMEM)


def rope_tables(length):
    half = HEAD_SIZE // 2
    freq = np.arange(half, dtype=np.float32)
    inverse = np.power(np.float32(ROPE_BASE), np.float32(-2.0) * freq / np.float32(HEAD_SIZE)).astype(np.float32)
    angles = np.arange(length, dtype=np.float32)[:, None] * inverse[None, :]
    cos, sin = np.cos(angles), np.sin(angles)
    return np.stack([
        np.concatenate([cos, cos], -1).astype(np.float32),
        np.concatenate([-sin, sin], -1).astype(np.float32),
    ])


def early_pieces(sec, ns):
    pairs = ns // 2
    count = PIECES * jnp.maximum(pairs - 1 - sec // 2, 0) // pairs if pairs else 0 * sec
    first = jnp.where((sec > 0) & (sec + 2 == ns), 1, 0)
    return jnp.where((sec % 2 == 1) & (sec + 1 < ns), count, first)


def kernel(
    n, ns,
    slot_ref, stash_ref, doc_hbm, gain_hbm, table_hbm, wq_ref, wk_ref, wv_ref,
    out_ref,
    raw, mine, dmine, w, xbuf, zbuf, dbuf, acc, q, k, v, dcol, drow, s_buf, p_buf,
    raw_sem, w_sem, hop_send, left_send, recv, zleft_send, zrecv,
    dshift_send, dleft_send, drecv,
    doc_ref, gain_ref, table, small_sem,
):
    me = lax.axis_index("tp")
    sec = lax.axis_index("section")
    slots, rows, width = raw.shape
    pieces = PIECES
    part = width // pieces
    nq, nk = wq_ref.shape[1], wk_ref.shape[1]
    total_n = w.shape[2]
    total = n * rows
    hold = n > 2
    even = sec % 2 == 0
    at_end = (me == 0) | (me == n - 1)
    has_right, has_left = me + 1 < n, me > 0
    has_next, has_prev = sec + 1 < ns, sec > 0
    early, early_prev = early_pieces(sec, ns), early_pieces(sec - 1, ns)

    starts = range(0, rows, CHUNK)
    raw_copies = [
        pltpu.make_async_copy(stash_ref.at[0, j, pl.ds(r, CHUNK)], raw.at[j, pl.ds(r, CHUNK)], raw_sem.at[i])
        for i, r in enumerate(starts) for j in range(slots)
    ]
    small = [
        pltpu.make_async_copy(src, dst, small_sem.at[i])
        for i, (src, dst) in enumerate(
            ((gain_hbm, gain_ref), (doc_hbm, doc_ref), (table_hbm, table))
        )
    ]
    for c in small[:1] + raw_copies + small[1:]:
        c.start()

    bar = pltpu.get_barrier_semaphore()
    for cond, target in (
        (has_right, {"tp": me + 1}),
        (has_left, {"tp": me - 1}),
        (has_next, {"section": sec + 1}),
        (has_prev, {"section": sec - 1}),
    ):
        @pl.when(cond)
        def _():
            pl.semaphore_signal(bar, inc=1, device_id=target, device_id_type=MESH)

    def w_copies():
        for p in range(pieces):
            span = pl.ds(p * part, part)
            yield pltpu.make_async_copy(wq_ref.at[span], w.at[p, :, 0:nq], w_sem)
            yield pltpu.make_async_copy(wk_ref.at[span], w.at[p, :, nq:nq + nk], w_sem)
            yield pltpu.make_async_copy(wv_ref.at[span], w.at[p, :, nq + nk:total_n], w_sem)

    for c in small[:1]:
        c.wait()
    chosen = slot_ref[0]
    for i, r in enumerate(starts):
        here = raw.at[:, pl.ds(r, CHUNK)]
        pltpu.make_async_copy(here, here, raw_sem.at[i]).wait()
        if i == len(starts) - 1:
            @pl.when(has_prev)
            def _():
                for c in w_copies():
                    c.start()
        x = raw[0, r:r + CHUNK, :]
        for j in range(1, slots):
            x = jnp.where(jnp.full(x.shape, chosen, jnp.int32) == j, raw[j, r:r + CHUNK, :], x)
        x = x.astype(jnp.float32)
        scale = lax.rsqrt(jnp.mean(x * x, axis=-1, keepdims=True) + NORM_EPSILON)
        y = (x * scale * gain_ref[...].astype(jnp.float32)[None, :]).astype(jnp.bfloat16)
        for p in range(pieces):
            mine[p, r:r + CHUNK, :] = y[:, p * part:(p + 1) * part]
    dmine[...] = jnp.zeros_like(dmine)
    for c in small[1:]:
        c.wait()
    docs = doc_ref[0, 0:1, :]
    for i in range(1, slots):
        docs = jnp.where(jnp.full(docs.shape, chosen, jnp.int32) == i, doc_ref[0, i:i + 1, :], docs)
    dmine[0:1, 0:rows] = docs

    def edges(a):
        return a.astype(jnp.int32)

    pl.semaphore_wait(bar, edges(has_right) + edges(has_left) + edges(has_next) + edges(has_prev))

    def remote(src, dst, ss, rs, target):
        return pltpu.make_async_remote_copy(
            src_ref=src, dst_ref=dst, send_sem=ss, recv_sem=rs, device_id=target, device_id_type=MESH
        )

    def sent(count, sem):
        for m in range(1, pieces + 1):
            @pl.when(count == m)
            def _():
                b = xbuf.at[0, pl.ds(0, m)]
                remote(b, b, sem, sem, {"section": sec}).wait_send()

    def hop(src, c, p):
        return remote(src, xbuf.at[c, p], hop_send.at[c], recv.at[c, p], {"section": sec + 1})

    def shift(p):
        return hop(mine.at[p], me, p)

    def zright(src, c, p):
        return remote(src, zbuf.at[c, p], zrecv.at[c, p], zrecv.at[c, p], {"tp": me + 1})

    def zleft(src, c, p, own=False):
        return remote(src, zbuf.at[c, p], zleft_send if own else zrecv.at[c, p], zrecv.at[c, p], {"tp": me - 1})

    def dshift():
        return remote(dmine, dbuf.at[me], dshift_send, drecv.at[me], {"section": sec + 1})

    def right(c, p):
        b = xbuf.at[c, p]
        return remote(b, b, recv.at[c, p], recv.at[c, p], {"tp": me + 1})

    def left(c, p, own=False):
        b = xbuf.at[c, p]
        return remote(b, b, left_send if own else recv.at[c, p], recv.at[c, p], {"tp": me - 1})

    def dright(c):
        b = dbuf.at[c]
        return remote(b, b, drecv.at[c], drecv.at[c], {"tp": me + 1})

    def dleft(c, own=False):
        b = dbuf.at[c]
        return remote(b, b, dleft_send if own else drecv.at[c], drecv.at[c], {"tp": me - 1})

    def both_ways(cond_right, cond_left, go_right, go_left):
        low = 2 * me < n

        @pl.when(cond_left & low)
        def _():
            go_left()

        @pl.when(cond_right)
        def _():
            go_right()

        @pl.when(cond_left & jnp.logical_not(low))
        def _():
            go_left()

    @pl.when(has_next)
    def _():
        dshift().start()
        for p in range(pieces - 1):
            both_ways(
                has_right & (p < early), has_left & (p < early),
                lambda: zright(mine.at[p], me, p).start(), lambda: zleft(mine.at[p], me, p, True).start(),
            )

        for p in range(pieces):
            shift(p).start()

    tile = 256

    def compute(c, p, last):
        x = xbuf[c, p]
        for t in range(0, total_n, tile):
            acc[c, :, t:t + tile] += jnp.dot(x, w[p, :, t:t + tile], preferred_element_type=jnp.float32)

        if last is False:
            return

        @pl.when(last)
        def _():
            span = pl.ds(pl.multiple_of(c * rows, rows), rows)
            cos, sin = table[0, span, :], table[1, span, :]
            for h in range(0, nq + nk, HEAD_SIZE):
                u = acc[c, :, h:h + HEAD_SIZE]
                u = (u * cos + pltpu.roll(u, HEAD_SIZE // 2, 1) * sin).astype(jnp.bfloat16)
                if h < nq:
                    q[span, h:h + HEAD_SIZE] = u
                else:
                    k[span, h - nq:h - nq + HEAD_SIZE] = u
            v[span, :] = acc[c, :, nq + nk:total_n].astype(jnp.bfloat16)

    heads = nk // HEAD_SIZE
    group = nq // nk
    factor = math.log2(math.e) / math.sqrt(HEAD_SIZE)

    def attend(i):
        span = pl.ds(pl.multiple_of(i * rows, rows), rows)
        lane_docs = jnp.concatenate([drow[c, 0:1, 0:rows] for c in range(n)], axis=1).astype(jnp.float32)
        i_idx = lax.broadcasted_iota(jnp.int32, (rows, total), 0) + i * rows
        j_idx = lax.broadcasted_iota(jnp.int32, (rows, total), 1)
        allowed = (j_idx <= i_idx) & (dcol[span, 0:1] == lane_docs)
        for g in range(heads):
            cols = slice(g * HEAD_SIZE, (g + 1) * HEAD_SIZE)
            qs = jnp.concatenate(
                [q[span, h * HEAD_SIZE:(h + 1) * HEAD_SIZE] for h in range(g * group, (g + 1) * group)], axis=0
            )
            scores = lax.dot_general(
                qs, k[:, cols], (((1,), (1,)), ((), ())), preferred_element_type=jnp.float32
            )
            for h in range(group):
                s_buf[g, h * rows:(h + 1) * rows, :] = jnp.where(
                    allowed, scores[h * rows:(h + 1) * rows], -1e30
                )
        for g in range(heads):
            for h in range(group):
                x = s_buf[g, h * rows:(h + 1) * rows, :]
                e = jnp.exp2((x - jnp.max(x, axis=-1, keepdims=True)) * factor)
                p_buf[g, h * rows:(h + 1) * rows, :] = e.astype(jnp.bfloat16)
        for g in range(heads):
            vg = v[:, g * HEAD_SIZE:(g + 1) * HEAD_SIZE]
            vg = jnp.concatenate([vg, jnp.ones_like(vg)], axis=1)
            both = jnp.dot(p_buf[g], vg, preferred_element_type=jnp.float32)
            both = (both[:, 0:HEAD_SIZE] / both[:, HEAD_SIZE:]).astype(jnp.bfloat16)
            for h in range(group):
                at = (g * group + h) * HEAD_SIZE
                out_ref[0, span, at:at + HEAD_SIZE] = both[h * rows:(h + 1) * rows]

    def attend_range(low, high):
        @pl.loop(low, high)
        def _(i):
            attend(i)

    def own_forward(p):
        held = (me == n - 2) & (p >= pieces - HELD) if hold else jnp.bool_(False)

        both_ways(
            has_right & (p >= early_prev) & jnp.logical_not(held), has_left & (p >= early_prev),
            lambda: right(me, p).start(), lambda: left(me, p, True).start(),
        )

    def weights_here():
        pltpu.make_async_copy(w, w, w_sem).wait()

    def keep_docs(c):
        drow[c] = dbuf[c]
        lanes = dbuf.shape[2]
        wide = jnp.broadcast_to(dbuf[c, 0:1, :].astype(jnp.float32), (lanes, lanes))
        dcol[pl.ds(pl.multiple_of(c * rows, rows), rows), :] = wide.T[0:rows, :]

    def pass_early(d, p):
        below, above = me - d, me + d

        @pl.when(below >= 0)
        def _():
            b = zbuf.at[below, p]
            zright(b, below, p).wait_recv()

            @pl.when(has_right)
            def _():
                zright(b, below, p).start()

            hop(b, below, p).start()

        @pl.when(above < n)
        def _():
            b = zbuf.at[above, p]
            zleft(b, above, p).wait_recv()

            @pl.when(has_left)
            def _():
                zleft(b, above, p).start()

            hop(b, above, p).start()

    def pass_all(d):
        if n > 1:
            @pl.loop(0, pieces - 1)
            def _(e):
                @pl.when(e < early)
                def _():
                    pass_early(d, e)

    @pl.when(has_prev)
    def _():
        acc[...] = jnp.zeros_like(acc)
        k[...] = jnp.zeros_like(k)
        v[...] = jnp.zeros_like(v)
        drow[...] = jnp.zeros_like(drow)

        dshift().wait_recv()

        @pl.when(has_right)
        def _():
            dright(me).start()

        @pl.when(has_left)
        def _():
            dleft(me, True).start()

        keep_docs(me)

        @pl.loop(0, pieces)
        def _(p):
            shift(p).wait_recv()
            own_forward(p)

            @pl.when(p == jnp.where(even, 0, pieces - 1))
            def _():
                pass_all(1)

        @pl.when(at_end)
        def _():
            weights_here()

            @pl.loop(0, pieces)
            def _(p):
                compute(me, p, p == pieces - 1)

        attend_range(0, jnp.where((me == 0) & (n > 1), 1, 0))

    def take_early(below, above):
        @pl.loop(0, 2 * pieces)
        def _(i):
            c = jnp.where(i < pieces, below, above)
            p = i % pieces

            @pl.when((c >= 0) & (c < n) & (p < early_prev))
            def _():
                hop(xbuf.at[c, p], c, p).wait_recv()
                compute(c, p, False)

    def drain():
        @pl.when(has_prev)
        def _():
            @pl.when(has_right)
            def _():
                dright(me).wait_send()
                for p in range(pieces):
                    @pl.when(p >= early_prev)
                    def _():
                        right(me, p).wait_send()

            @pl.when(has_left)
            def _():
                dleft(me, True).wait_send()
                sent(pieces - early_prev, left_send)

            for d in range(1, n):
                below, above = me - d, me + d

                @pl.when((below >= 0) & has_right)
                def _():
                    dright(below).wait_send()
                    for p in range(pieces):
                        @pl.when(p >= early_prev)
                        def _():
                            right(below, p).wait_send()

                @pl.when((above < n) & has_left)
                def _():
                    dleft(above).wait_send()
                    for p in range(pieces):
                        @pl.when(p >= early_prev)
                        def _():
                            left(above, p).wait_send()

        @pl.when(has_next)
        def _():
            dshift().wait_send()
            sent(pieces, hop_send.at[me])

            @pl.when(early > 0)
            def _():
                @pl.when(has_left)
                def _():
                    sent(early, zleft_send)

                @pl.when(has_right)
                def _():
                    for p in range(pieces - 1):
                        @pl.when(p < early)
                        def _():
                            zright(mine.at[p], me, p).wait_send()

                for d in range(1, n):
                    below, above = me - d, me + d

                    @pl.when(below >= 0)
                    def _():
                        sent(early, hop_send.at[below])

                        @pl.when(has_right)
                        def _():
                            for p in range(pieces - 1):
                                @pl.when(p < early)
                                def _():
                                    zright(zbuf.at[below, p], below, p).wait_send()

                    @pl.when(above < n)
                    def _():
                        sent(early, hop_send.at[above])

                        @pl.when(has_left)
                        def _():
                            for p in range(pieces - 1):
                                @pl.when(p < early)
                                def _():
                                    zleft(zbuf.at[above, p], above, p).wait_send()

    @pl.when(has_prev)
    def _():
        @pl.loop(0, (n - 1) * pieces)
        def _(i):
            d, p = i // pieces + 1, i % pieces
            below, above = me - d, me + d
            late = p >= early_prev
            final = p == pieces - 1
            from_left = late & (below >= 0)
            if hold:
                from_left = from_left & jnp.logical_not((me == n - 1) & (d == 1) & (p >= pieces - HELD))

            @pl.when(jnp.where(even, (p == pieces - 1) & (d < n - 1), (p == 0) & (d > 1)))
            def _():
                pass_all(jnp.where(even, d + 1, d))

            @pl.when((below >= 0) & (p == 0))
            def _():
                dright(below).wait_recv()

                @pl.when(has_right)
                def _():
                    dright(below).start()

                keep_docs(below)

            @pl.when((above < n) & (p == 0))
            def _():
                dleft(above).wait_recv()

                @pl.when(has_left)
                def _():
                    dleft(above).start()

                keep_docs(above)

            @pl.when((p == pieces - 2) & (d == n - 1))
            def _():
                @pl.when(at_end)
                def _():
                    drain()

                take_early(below, above)

            @pl.when(from_left)
            def _():
                right(below, p).wait_recv()

                @pl.when(has_right)
                def _():
                    right(below, p).start()

            if hold:
                @pl.when((me == n - 2) & (d == n - 2) & final)
                def _():
                    for t in range(pieces - HELD, pieces):
                        @pl.when(t >= early_prev)
                        def _():
                            right(me, t).start()

            @pl.when(late & (above < n))
            def _():
                left(above, p).wait_recv()

                @pl.when(has_left)
                def _():
                    left(above, p).start()

            @pl.when((i == 0) & jnp.logical_not(at_end))
            def _():
                weights_here()

            @pl.when(final & (d < n - 1))
            def _():
                take_early(below, above)

            @pl.when((d == min(2, n - 1)) & jnp.logical_not(at_end))
            def _():
                compute(me, p, final)

            @pl.when(from_left)
            def _():
                compute(below, p, final)

            @pl.when(late & (above < n))
            def _():
                compute(above, p, final)

            @pl.when(final & (me == 0) & (d < n - 1))
            def _():
                attend(d)

        if hold:
            @pl.when(me == n - 1)
            def _():
                attend_range(0, n - 2)

                @pl.loop(pieces - HELD, pieces)
                def _(p):
                    @pl.when(p >= early_prev)
                    def _():
                        right(n - 2, p).wait_recv()
                        compute(n - 2, p, p == pieces - 1)

        attend_range(jnp.where(me == 0, n - 1, jnp.where(me == n - 1, max(n - 2, 0), 0)), n)

    @pl.when(jnp.logical_not(has_prev & at_end))
    def _():
        drain()

    @pl.when(jnp.logical_not(has_prev))
    def _():
        out_ref[...] = jnp.zeros_like(out_ref)


def in_hbm(a):
    return pltpu.with_memory_space_constraint(a, pltpu.HBM)


def per_device(stash, slot, doc_ids, norm_gain, w_query, w_key, value_weight):
    n, ns = lax.axis_size("tp"), lax.axis_size("section")
    _, slots, rows, width = stash.shape
    total = n * rows
    nq, nk = w_query.shape[1], w_key.shape[1]
    total_n = nq + nk + value_weight.shape[1]
    table = rope_tables(total)
    lanes = -(-rows // 128) * 128
    bf, f32, dma = jnp.bfloat16, jnp.float32, pltpu.SemaphoreType.DMA
    part = width // PIECES
    heads, stacked = nk // HEAD_SIZE, nq // nk * rows
    operands = (stash, doc_ids, norm_gain, jnp.asarray(table), w_query, w_key, value_weight)
    return pl.pallas_call(
        functools.partial(kernel, n, ns),
        out_shape=jax.ShapeDtypeStruct((1, total, nq), bf),
        in_specs=[pl.BlockSpec(memory_space=pltpu.SMEM)] + [ANY] * 7,
        out_specs=VMEM,
        scratch_shapes=[
            pltpu.VMEM((slots, rows, width), bf),
            pltpu.VMEM((PIECES, rows, part), bf),
            pltpu.VMEM((8, lanes), jnp.int32),
            pltpu.VMEM((PIECES, part, total_n), bf),
            pltpu.VMEM((n, PIECES, rows, part), bf),
            pltpu.VMEM((n, PIECES - 1, rows, part), bf),
            pltpu.VMEM((n, 8, lanes), jnp.int32),
            pltpu.VMEM((n, rows, total_n), f32),
            pltpu.VMEM((total, nq), bf),
            pltpu.VMEM((total, nk), bf),
            pltpu.VMEM((total, nk), bf),
            pltpu.VMEM((total, lanes), f32),
            pltpu.VMEM((n, 8, lanes), jnp.int32),
            pltpu.VMEM((heads, stacked, total), f32),
            pltpu.VMEM((heads, stacked, total), bf),
            dma((rows // CHUNK,)),
            dma,
            dma((n,)),
            dma,
            dma((n, PIECES)),
            dma,
            dma((n, PIECES - 1)),
            dma,
            dma,
            dma((n,)),
            pltpu.VMEM(doc_ids.shape, jnp.int32),
            pltpu.VMEM(norm_gain.shape, bf),
            pltpu.VMEM(table.shape, f32),
            dma((3,)),
        ],
        compiler_params=pltpu.CompilerParams(
            collective_id=0, has_side_effects=True, vmem_limit_bytes=VMEM_GRANT
        ),
        cost_estimate=pl.CostEstimate(
            flops=2 * total * width * total_n, bytes_accessed=width * total_n * 2, transcendentals=0
        ),
    )(slot, *(in_hbm(a) for a in operands))


def solution(mesh):
    placed = (
        P("section", None, "tp", None),
        P("section"),
        P("section", None, "tp"),
        P(),
        P(None, "tp"),
        P(None, "tp"),
        P(None, "tp"),
    )
    return jax.shard_map(
        per_device, mesh=mesh, in_specs=placed, out_specs=P("section", None, "tp"), check_vma=False
    )
```

```python
import functools
import math

import jax
import jax.numpy as jnp
import numpy as np
from jax import lax
from jax.experimental import pallas as pl
from jax.experimental.pallas import tpu as pltpu
from jax.sharding import PartitionSpec as P

HEAD_SIZE = 128
ROPE_BASE = 500000.0
NORM_EPSILON = 1e-05
PIECES = 4
HELD = 1
CHUNK = 16
MESH = pl.DeviceIdType.MESH
VMEM_GRANT = 32 << 20
ANY = pl.BlockSpec(memory_space=pltpu.HBM)
VMEM = pl.BlockSpec(memory_space=pltpu.VMEM)


def rope_tables(length):
    half = HEAD_SIZE // 2
    freq = np.arange(half, dtype=np.float32)
    inverse = np.power(np.float32(ROPE_BASE), np.float32(-2.0) * freq / np.float32(HEAD_SIZE)).astype(np.float32)
    angles = np.arange(length, dtype=np.float32)[:, None] * inverse[None, :]
    cos, sin = np.cos(angles), np.sin(angles)
    return np.stack([
        np.concatenate([cos, cos], -1).astype(np.float32),
        np.concatenate([-sin, sin], -1).astype(np.float32),
    ])


def early_pieces(sec, ns):
    pairs = ns // 2
    count = PIECES * jnp.maximum(pairs - 1 - sec // 2, 0) // pairs if pairs else 0 * sec
    first = jnp.where((sec > 0) & (sec + 2 == ns), 1, 0)
    return jnp.where((sec % 2 == 1) & (sec + 1 < ns), count, first)


def kernel(
    n, ns,
    slot_ref, stash_ref, doc_hbm, gain_hbm, table_hbm, wq_ref, wk_ref, wv_ref,
    out_ref,
    raw, mine, dmine, w, xbuf, zbuf, dbuf, acc, q, k, v, dcol, drow, s_buf, p_buf,
    w_sem, hop_send, left_send, recv, recv2, zleft_send, zrecv,
    dshift_send, dleft_send, drecv, table_sem,
    doc_ref, gain_ref, table,
):
    me = lax.axis_index("tp")
    sec = lax.axis_index("section")
    slots, rows, width = raw.shape
    pieces = PIECES
    part = width // pieces
    half = part // 2
    nq, nk = wq_ref.shape[1], wk_ref.shape[1]
    total_n = w.shape[2]
    total = n * rows
    hold = n > 2
    even = sec % 2 == 0
    at_end = (me == 0) | (me == n - 1)
    has_right, has_left = me + 1 < n, me > 0
    has_next, has_prev = sec + 1 < ns, sec > 0
    early, early_prev = early_pieces(sec, ns), early_pieces(sec - 1, ns)

    starts = range(0, rows, CHUNK)
    raw_copies = [
        pltpu.make_async_copy(stash_ref.at[0, j, pl.ds(r, CHUNK)], raw.at[j, pl.ds(r, CHUNK)], hop_send.at[i])
        for i, r in enumerate(starts) for j in range(slots)
    ]
    gain_copy = pltpu.make_async_copy(gain_hbm, gain_ref, left_send)
    doc_copy = pltpu.make_async_copy(doc_hbm, doc_ref, zleft_send)
    table_copy = pltpu.make_async_copy(table_hbm, table, table_sem)
    for c in [gain_copy] + raw_copies + [doc_copy]:
        c.start()

    bar = pltpu.get_barrier_semaphore()
    for cond, target in (
        (has_right, {"tp": me + 1}),
        (has_left, {"tp": me - 1}),
        (has_next, {"section": sec + 1}),
        (has_prev, {"section": sec - 1}),
    ):
        @pl.when(cond)
        def _():
            pl.semaphore_signal(bar, inc=1, device_id=target, device_id_type=MESH)

    def w_copies():
        for p in range(2 * pieces):
            span = pl.ds(p * half, half)
            yield pltpu.make_async_copy(wq_ref.at[span], w.at[p, :, 0:nq], w_sem)
            yield pltpu.make_async_copy(wk_ref.at[span], w.at[p, :, nq:nq + nk], w_sem)
            yield pltpu.make_async_copy(wv_ref.at[span], w.at[p, :, nq + nk:total_n], w_sem)

    gain_copy.wait()
    chosen = slot_ref[0]
    for i, r in enumerate(starts):
        here = raw.at[:, pl.ds(r, CHUNK)]
        pltpu.make_async_copy(here, here, hop_send.at[i]).wait()
        if i == len(starts) - 1:
            @pl.when(has_prev)
            def _():
                table_copy.start()
                for c in w_copies():
                    c.start()
        x = raw[0, r:r + CHUNK, :]
        for j in range(1, slots):
            x = jnp.where(jnp.full(x.shape, chosen, jnp.int32) == j, raw[j, r:r + CHUNK, :], x)
        x = x.astype(jnp.float32)
        scale = lax.rsqrt(jnp.mean(x * x, axis=-1, keepdims=True) + NORM_EPSILON)
        y = (x * scale * gain_ref[...].astype(jnp.float32)[None, :]).astype(jnp.bfloat16)
        for p in range(2 * pieces):
            mine[p, r:r + CHUNK, :] = y[:, p * half:(p + 1) * half]
    dmine[...] = jnp.zeros_like(dmine)
    doc_copy.wait()
    docs = doc_ref[0, 0:1, :]
    for i in range(1, slots):
        docs = jnp.where(jnp.full(docs.shape, chosen, jnp.int32) == i, doc_ref[0, i:i + 1, :], docs)
    dmine[0:1, 0:rows] = docs

    def edges(a):
        return a.astype(jnp.int32)

    pl.semaphore_wait(bar, edges(has_right) + edges(has_left) + edges(has_next) + edges(has_prev))

    def remote(src, dst, ss, rs, target):
        return pltpu.make_async_remote_copy(
            src_ref=src, dst_ref=dst, send_sem=ss, recv_sem=rs, device_id=target, device_id_type=MESH
        )

    def sent(count, sem):
        for m in range(1, pieces + 1):
            @pl.when(count == m)
            def _():
                b = xbuf.at[0, pl.ds(0, 2 * m)]
                remote(b, b, sem, sem, {"section": sec}).wait_send()

    def whole(p):
        return pl.ds(2 * p, 2)

    def first():
        return pl.ds(2 * pieces - 2, 1)

    def second():
        return pl.ds(2 * pieces - 1, 1)

    def hop(src, c, p):
        return remote(src, xbuf.at[c, whole(p)], hop_send.at[c], recv.at[c, p], {"section": sec + 1})

    def shift(p):
        return hop(mine.at[whole(p)], me, p)

    def shift_last():
        return [
            remote(mine.at[at], xbuf.at[me, at], hop_send.at[me], rs, {"section": sec + 1})
            for at, rs in ((first(), recv.at[me, pieces - 1]), (second(), recv2.at[me]))
        ]

    def zright(src, c, p):
        return remote(src, zbuf.at[c, whole(p)], zrecv.at[c, p], zrecv.at[c, p], {"tp": me + 1})

    def zleft(src, c, p, own=False):
        return remote(
            src, zbuf.at[c, whole(p)], zleft_send if own else zrecv.at[c, p], zrecv.at[c, p], {"tp": me - 1}
        )

    def to_right(at, c, rs):
        b = xbuf.at[c, at]
        return remote(b, b, rs, rs, {"tp": me + 1})

    def to_left(at, c, rs, own=False):
        b = xbuf.at[c, at]
        return remote(b, b, left_send if own else rs, rs, {"tp": me - 1})

    def right(c, p):
        return to_right(whole(p), c, recv.at[c, p])

    def left(c, p, own=False):
        return to_left(whole(p), c, recv.at[c, p], own)

    def right_last(c):
        return [to_right(first(), c, recv.at[c, pieces - 1]), to_right(second(), c, recv2.at[c])]

    def left_last(c, own=False):
        return [to_left(first(), c, recv.at[c, pieces - 1], own), to_left(second(), c, recv2.at[c], own)]

    def each(copies, act):
        for c in copies:
            act(c)

    def pick(p, ordinary, last, act):
        @pl.when(p < pieces - 1)
        def _():
            act(ordinary())

        @pl.when(p == pieces - 1)
        def _():
            each(last(), act)

    def start(c):
        c.start()

    def wait_send(c):
        c.wait_send()

    def wait_recv(c):
        c.wait_recv()

    def dshift():
        return remote(dmine, dbuf.at[me], dshift_send, drecv.at[me], {"section": sec + 1})

    def dright(c):
        b = dbuf.at[c]
        return remote(b, b, drecv.at[c], drecv.at[c], {"tp": me + 1})

    def dleft(c, own=False):
        b = dbuf.at[c]
        return remote(b, b, dleft_send if own else drecv.at[c], drecv.at[c], {"tp": me - 1})

    def both_ways(cond_right, cond_left, go_right, go_left):
        low = 2 * me < n

        @pl.when(cond_left & low)
        def _():
            go_left()

        @pl.when(cond_right)
        def _():
            go_right()

        @pl.when(cond_left & jnp.logical_not(low))
        def _():
            go_left()

    @pl.when(has_next)
    def _():
        dshift().start()
        for p in range(pieces - 1):
            both_ways(
                has_right & (p < early), has_left & (p < early),
                lambda: zright(mine.at[whole(p)], me, p).start(),
                lambda: zleft(mine.at[whole(p)], me, p, True).start(),
            )

        for p in range(pieces - 1):
            shift(p).start()
        each(shift_last(), start)

    tile = 256

    def compute(c, p, last, halves=2):
        at = pl.ds(2 * p if halves == 2 else p, halves)
        x = xbuf[c, at]
        x = jnp.concatenate([x[j] for j in range(halves)], axis=1)
        for t in range(0, total_n, tile):
            wt = w[at, :, t:t + tile].reshape(halves * half, tile)
            acc[c, :, t:t + tile] += jnp.dot(x, wt, preferred_element_type=jnp.float32)

        if last is False:
            return

        @pl.when(last)
        def _():
            span = pl.ds(pl.multiple_of(c * rows, rows), rows)
            cos, sin = table[0, span, :], table[1, span, :]
            for h in range(0, nq + nk, HEAD_SIZE):
                u = acc[c, :, h:h + HEAD_SIZE]
                u = (u * cos + pltpu.roll(u, HEAD_SIZE // 2, 1) * sin).astype(jnp.bfloat16)
                if h < nq:
                    q[span, h:h + HEAD_SIZE] = u
                else:
                    k[span, h - nq:h - nq + HEAD_SIZE] = u
            v[span, :] = acc[c, :, nq + nk:total_n].astype(jnp.bfloat16)

    heads = nk // HEAD_SIZE
    group = nq // nk
    factor = math.log2(math.e) / math.sqrt(HEAD_SIZE)

    def attend(i):
        span = pl.ds(pl.multiple_of(i * rows, rows), rows)
        lane_docs = jnp.concatenate([drow[c, 0:1, 0:rows] for c in range(n)], axis=1).astype(jnp.float32)
        i_idx = lax.broadcasted_iota(jnp.int32, (rows, total), 0) + i * rows
        j_idx = lax.broadcasted_iota(jnp.int32, (rows, total), 1)
        allowed = (j_idx <= i_idx) & (dcol[span, 0:1] == lane_docs)
        for g in range(heads):
            cols = slice(g * HEAD_SIZE, (g + 1) * HEAD_SIZE)
            qs = jnp.concatenate(
                [q[span, h * HEAD_SIZE:(h + 1) * HEAD_SIZE] for h in range(g * group, (g + 1) * group)], axis=0
            )
            scores = lax.dot_general(
                qs, k[:, cols], (((1,), (1,)), ((), ())), preferred_element_type=jnp.float32
            )
            for h in range(group):
                s_buf[g, h * rows:(h + 1) * rows, :] = jnp.where(
                    allowed, scores[h * rows:(h + 1) * rows], -1e30
                )
        for g in range(heads):
            for h in range(group):
                x = s_buf[g, h * rows:(h + 1) * rows, :]
                e = jnp.exp2((x - jnp.max(x, axis=-1, keepdims=True)) * factor)
                p_buf[g, h * rows:(h + 1) * rows, :] = e.astype(jnp.bfloat16)
        for g in range(heads):
            vg = v[:, g * HEAD_SIZE:(g + 1) * HEAD_SIZE]
            vg = jnp.concatenate([vg, jnp.ones_like(vg)], axis=1)
            both = jnp.dot(p_buf[g], vg, preferred_element_type=jnp.float32)
            both = (both[:, 0:HEAD_SIZE] / both[:, HEAD_SIZE:]).astype(jnp.bfloat16)
            for h in range(group):
                at = (g * group + h) * HEAD_SIZE
                out_ref[0, span, at:at + HEAD_SIZE] = both[h * rows:(h + 1) * rows]

    def attend_range(low, high):
        @pl.loop(low, high)
        def _(i):
            attend(i)

    def own_forward(p):
        held = (me == n - 2) & (p >= pieces - HELD) if hold else jnp.bool_(False)

        both_ways(
            has_right & (p >= early_prev) & jnp.logical_not(held), has_left & (p >= early_prev),
            lambda: pick(p, lambda: right(me, p), lambda: right_last(me), start),
            lambda: pick(p, lambda: left(me, p, True), lambda: left_last(me, True), start),
        )

    def weights_here():
        table_copy.wait()
        pltpu.make_async_copy(w, w, w_sem).wait()

    def keep_docs(c):
        drow[c] = dbuf[c]
        lanes = dbuf.shape[2]
        wide = jnp.broadcast_to(dbuf[c, 0:1, :].astype(jnp.float32), (lanes, lanes))
        dcol[pl.ds(pl.multiple_of(c * rows, rows), rows), :] = wide.T[0:rows, :]

    def pass_early(d, p):
        below, above = me - d, me + d

        @pl.when(below >= 0)
        def _():
            b = zbuf.at[below, whole(p)]
            zright(b, below, p).wait_recv()

            @pl.when(has_right)
            def _():
                zright(b, below, p).start()

            hop(b, below, p).start()

        @pl.when(above < n)
        def _():
            b = zbuf.at[above, whole(p)]
            zleft(b, above, p).wait_recv()

            @pl.when(has_left)
            def _():
                zleft(b, above, p).start()

            hop(b, above, p).start()

    def pass_all(d):
        if n > 1:
            @pl.loop(0, pieces - 1)
            def _(e):
                @pl.when(e < early)
                def _():
                    pass_early(d, e)

    @pl.when(has_prev)
    def _():
        acc[...] = jnp.zeros_like(acc)
        k[...] = jnp.zeros_like(k)
        v[...] = jnp.zeros_like(v)
        drow[...] = jnp.zeros_like(drow)

        dshift().wait_recv()

        @pl.when(has_right)
        def _():
            dright(me).start()

        @pl.when(has_left)
        def _():
            dleft(me, True).start()

        keep_docs(me)

        @pl.loop(0, pieces)
        def _(p):
            pick(p, lambda: shift(p), shift_last, wait_recv)
            own_forward(p)

            @pl.when(p == jnp.where(even, 0, pieces - 1))
            def _():
                pass_all(1)

        @pl.when(at_end)
        def _():
            weights_here()

            @pl.loop(0, pieces)
            def _(p):
                compute(me, p, p == pieces - 1)

        attend_range(0, jnp.where((me == 0) & (n > 1), 1, 0))

    def take_early(c):
        @pl.loop(0, pieces - 1)
        def _(p):
            @pl.when(p < early_prev)
            def _():
                hop(xbuf.at[c, whole(p)], c, p).wait_recv()
                compute(c, p, False)

    def drain():
        @pl.when(has_prev)
        def _():
            @pl.when(has_right)
            def _():
                dright(me).wait_send()
                for p in range(pieces - 1):
                    @pl.when(p >= early_prev)
                    def _():
                        right(me, p).wait_send()
                each(right_last(me), wait_send)

            @pl.when(has_left)
            def _():
                dleft(me, True).wait_send()
                sent(pieces - early_prev, left_send)

            for d in range(1, n):
                below, above = me - d, me + d

                @pl.when((below >= 0) & has_right)
                def _():
                    dright(below).wait_send()
                    for p in range(pieces - 1):
                        @pl.when(p >= early_prev)
                        def _():
                            right(below, p).wait_send()
                    each(right_last(below), wait_send)

                @pl.when((above < n) & has_left)
                def _():
                    dleft(above).wait_send()
                    for p in range(pieces - 1):
                        @pl.when(p >= early_prev)
                        def _():
                            left(above, p).wait_send()
                    each(left_last(above), wait_send)

        @pl.when(has_next)
        def _():
            dshift().wait_send()
            sent(pieces, hop_send.at[me])

            @pl.when(early > 0)
            def _():
                @pl.when(has_left)
                def _():
                    sent(early, zleft_send)

                @pl.when(has_right)
                def _():
                    for p in range(pieces - 1):
                        @pl.when(p < early)
                        def _():
                            zright(mine.at[whole(p)], me, p).wait_send()

                for d in range(1, n):
                    below, above = me - d, me + d

                    @pl.when(below >= 0)
                    def _():
                        sent(early, hop_send.at[below])

                        @pl.when(has_right)
                        def _():
                            for p in range(pieces - 1):
                                @pl.when(p < early)
                                def _():
                                    zright(zbuf.at[below, whole(p)], below, p).wait_send()

                    @pl.when(above < n)
                    def _():
                        sent(early, hop_send.at[above])

                        @pl.when(has_left)
                        def _():
                            for p in range(pieces - 1):
                                @pl.when(p < early)
                                def _():
                                    zleft(zbuf.at[above, whole(p)], above, p).wait_send()

    def take_last(c):
        for t, r in enumerate(right_last(c)):
            r.wait_recv()
            compute(c, 2 * pieces - 2 + t, jnp.bool_(t == 1), 1)

    def pass_now(d, p):
        @pl.when(jnp.where(even, (p == pieces - 1) & (d < n - 1), (p == 0) & (d > 1)))
        def _():
            pass_all(jnp.where(even, d + 1, d))

    @pl.when(has_prev & at_end)
    def _():
        drain_at = jnp.where(even & (n > 2), (n - 3) * pieces + pieces - 1, (n - 2) * pieces + 1)
        ahead = (early_prev == 1) & (n > 2)

        @pl.loop(0, (n - 1) * pieces)
        def _(i):
            d, p = i // pieces + 1, i % pieces
            c = jnp.where(me == 0, d, n - 1 - d)
            go = p >= early_prev
            if hold:
                go = go & jnp.logical_not((me == n - 1) & (d == 1) & (p >= pieces - HELD))

            pass_now(d, p)

            @pl.when(p == 0)
            def _():
                dright(c).wait_recv()
                keep_docs(c)

            @pl.when(i == drain_at)
            def _():
                drain()

            sooner = ahead & (d == n - 2) & (p == pieces - 1)
            usual = (p == pieces - 2) & jnp.logical_not(ahead & (d == n - 1))

            @pl.when((early_prev > 0) & (sooner | usual))
            def _():
                take_early(jnp.where(sooner, jnp.where(me == 0, n - 1, 0), c))

            @pl.when(go & (p < pieces - 1))
            def _():
                right(c, p).wait_recv()
                compute(c, p, False)

            @pl.when(go & (p == pieces - 1))
            def _():
                take_last(c)

            @pl.when((p == pieces - 1) & (me == 0) & (d < n - 1))
            def _():
                attend(d)

        if hold:
            @pl.when(me == n - 1)
            def _():
                attend_range(0, n - 2)

                for p in range(pieces - HELD, pieces - 1):
                    @pl.when(p >= early_prev)
                    def _():
                        right(n - 2, p).wait_recv()
                        compute(n - 2, p, False)

                take_last(n - 2)

    @pl.when(has_prev & jnp.logical_not(at_end))
    def _():
        @pl.loop(0, (n - 1) * pieces)
        def _(i):
            d, p = i // pieces + 1, i % pieces
            below, above = me - d, me + d
            late = p >= early_prev
            final = p == pieces - 1

            pass_now(d, p)

            @pl.when((below >= 0) & (p == 0))
            def _():
                dright(below).wait_recv()
                dright(below).start()
                keep_docs(below)

            @pl.when((above < n) & (p == 0))
            def _():
                dleft(above).wait_recv()
                dleft(above).start()
                keep_docs(above)

            def forward(c):
                c.wait_recv()
                c.start()

            @pl.when(late & (below >= 0))
            def _():
                pick(p, lambda: right(below, p), lambda: right_last(below), forward)

            if hold:
                @pl.when((me == n - 2) & (d == n - 2) & final)
                def _():
                    for t in range(pieces - HELD, pieces - 1):
                        @pl.when(t >= early_prev)
                        def _():
                            right(me, t).start()
                    each(right_last(me), start)

            @pl.when(late & (above < n))
            def _():
                pick(p, lambda: left(above, p), lambda: left_last(above), forward)

            @pl.when(i == 0)
            def _():
                weights_here()

            @pl.when((p == pieces - 2) & (early_prev > 0))
            def _():
                @pl.when(below >= 0)
                def _():
                    take_early(below)

                @pl.when(above < n)
                def _():
                    take_early(above)

            @pl.when(d == min(2, n - 1))
            def _():
                compute(me, p, final)

            @pl.when(late & (below >= 0))
            def _():
                compute(below, p, final)

            @pl.when(late & (above < n))
            def _():
                compute(above, p, final)

    @pl.when(has_prev)
    def _():
        attend_range(jnp.where(me == 0, n - 1, jnp.where(me == n - 1, max(n - 2, 0), 0)), n)

    @pl.when(jnp.logical_not(has_prev & at_end))
    def _():
        drain()

    @pl.when(jnp.logical_not(has_prev))
    def _():
        out_ref[...] = jnp.zeros_like(out_ref)


def in_hbm(a):
    return pltpu.with_memory_space_constraint(a, pltpu.HBM)


def per_device(stash, slot, doc_ids, norm_gain, w_query, w_key, value_weight):
    n, ns = lax.axis_size("tp"), lax.axis_size("section")
    _, slots, rows, width = stash.shape
    total = n * rows
    nq, nk = w_query.shape[1], w_key.shape[1]
    total_n = nq + nk + value_weight.shape[1]
    table = rope_tables(total)
    lanes = -(-rows // 128) * 128
    bf, f32, dma = jnp.bfloat16, jnp.float32, pltpu.SemaphoreType.DMA
    part = width // PIECES
    heads, stacked = nk // HEAD_SIZE, nq // nk * rows
    operands = (stash, doc_ids, norm_gain, jnp.asarray(table), w_query, w_key, value_weight)
    return pl.pallas_call(
        functools.partial(kernel, n, ns),
        out_shape=jax.ShapeDtypeStruct((1, total, nq), bf),
        in_specs=[pl.BlockSpec(memory_space=pltpu.SMEM)] + [ANY] * 7,
        out_specs=VMEM,
        scratch_shapes=[
            pltpu.VMEM((slots, rows, width), bf),
            pltpu.VMEM((2 * PIECES, rows, part // 2), bf),
            pltpu.VMEM((8, lanes), jnp.int32),
            pltpu.VMEM((2 * PIECES, part // 2, total_n), bf),
            pltpu.VMEM((n, 2 * PIECES, rows, part // 2), bf),
            pltpu.VMEM((n, 2 * PIECES - 2, rows, part // 2), bf),
            pltpu.VMEM((n, 8, lanes), jnp.int32),
            pltpu.VMEM((n, rows, total_n), f32),
            pltpu.VMEM((total, nq), bf),
            pltpu.VMEM((total, nk), bf),
            pltpu.VMEM((total, nk), bf),
            pltpu.VMEM((total, lanes), f32),
            pltpu.VMEM((n, 8, lanes), jnp.int32),
            pltpu.VMEM((heads, stacked, total), f32),
            pltpu.VMEM((heads, stacked, total), bf),
            dma,
            dma((max(n, rows // CHUNK),)),
            dma,
            dma((n, PIECES)),
            dma((n,)),
            dma,
            dma((n, PIECES - 1)),
            dma,
            dma,
            dma((n,)),
            dma,
            pltpu.VMEM(doc_ids.shape, jnp.int32),
            pltpu.VMEM(norm_gain.shape, bf),
            pltpu.VMEM(table.shape, f32),
        ],
        compiler_params=pltpu.CompilerParams(
            collective_id=0, has_side_effects=True, vmem_limit_bytes=VMEM_GRANT
        ),
        cost_estimate=pl.CostEstimate(
            flops=2 * total * width * total_n, bytes_accessed=width * total_n * 2, transcendentals=0
        ),
    )(slot, *(in_hbm(a) for a in operands))


def solution(mesh):
    placed = (
        P("section", None, "tp", None),
        P("section"),
        P("section", None, "tp"),
        P(),
        P(None, "tp"),
        P(None, "tp"),
        P(None, "tp"),
    )
    return jax.shard_map(
        per_device, mesh=mesh, in_specs=placed, out_specs=P("section", None, "tp"), check_vma=False
    )
```

```python
import functools
import math

import jax
import jax.numpy as jnp
import numpy as np
from jax import lax
from jax.experimental import pallas as pl
from jax.experimental.pallas import tpu as pltpu
from jax.sharding import PartitionSpec as P

HEAD_SIZE = 128
ROPE_BASE = 500000.0
NORM_EPSILON = 1e-05
PIECES = 4
HELD = 1
CHUNK = 16
MESH = pl.DeviceIdType.MESH
VMEM_GRANT = 32 << 20
ANY = pl.BlockSpec(memory_space=pltpu.HBM)
VMEM = pl.BlockSpec(memory_space=pltpu.VMEM)


def rope_tables(length):
    half = HEAD_SIZE // 2
    freq = np.arange(half, dtype=np.float32)
    inverse = np.power(np.float32(ROPE_BASE), np.float32(-2.0) * freq / np.float32(HEAD_SIZE)).astype(np.float32)
    angles = np.arange(length, dtype=np.float32)[:, None] * inverse[None, :]
    cos, sin = np.cos(angles), np.sin(angles)
    return np.stack([
        np.concatenate([cos, cos], -1).astype(np.float32),
        np.concatenate([-sin, sin], -1).astype(np.float32),
    ])


def early_pieces(sec, ns):
    pairs = ns // 2
    count = PIECES * jnp.maximum(pairs - 1 - sec // 2, 0) // pairs if pairs else 0 * sec
    first = jnp.where((sec > 0) & (sec + 2 == ns), 1, 0)
    return jnp.where((sec % 2 == 1) & (sec + 1 < ns), count, first)


def kernel(
    n, ns,
    slot_ref, stash_ref, doc_hbm, gain_hbm, table_hbm, wq_ref, wk_ref, wv_ref,
    out_ref,
    raw, mine, dmine, w, xbuf, zbuf, dbuf, acc, q, k, v, dcol, drow, s_buf, p_buf,
    w_sem, hop_send, left_send, recv, recv2, zleft_send, zrecv,
    dshift_send, dleft_send, drecv, table_sem, ready,
    doc_ref, gain_ref, table,
):
    me = lax.axis_index("tp")
    sec = lax.axis_index("section")
    slots, rows, width = raw.shape
    pieces = PIECES
    part = width // pieces
    half = part // 2
    nq, nk = wq_ref.shape[1], wk_ref.shape[1]
    total_n = w.shape[2]
    total = n * rows
    hold = n > 2
    even, odd = sec % 2 == 0, sec % 2 == 1
    at_end = (me == 0) | (me == n - 1)
    has_right, has_left = me + 1 < n, me > 0
    has_next, has_prev = sec + 1 < ns, sec > 0
    early, early_prev = early_pieces(sec, ns), early_pieces(sec - 1, ns)
    greet, greet_prev = odd & (early >= 2), even & (early_prev >= 2)

    bar = pltpu.get_barrier_semaphore()
    for cond, target in (
        (has_right, {"tp": me + 1}),
        (has_left, {"tp": me - 1}),
        (has_next & greet, {"section": sec + 1}),
        (has_prev & jnp.logical_not(greet_prev), {"section": sec - 1}),
    ):
        @pl.when(cond)
        def _():
            pl.semaphore_signal(bar, inc=1, device_id=target, device_id_type=MESH)

    starts = range(0, rows, CHUNK)
    raw_copies = [pltpu.make_async_copy(stash_ref.at[0, :, pl.ds(r, CHUNK)], raw.at[:, pl.ds(r, CHUNK)], hop_send.at[0]) for r in starts]
    gain_copy = pltpu.make_async_copy(gain_hbm, gain_ref, left_send)
    doc_copy = pltpu.make_async_copy(doc_hbm, doc_ref, zleft_send)
    table_copy = pltpu.make_async_copy(table_hbm, table, table_sem)
    for c in raw_copies + [gain_copy, doc_copy]:
        c.start()

    def w_copies():
        for p in range(2 * pieces):
            span = pl.ds(p * half, half)
            yield pltpu.make_async_copy(wq_ref.at[span], w.at[p, :, 0:nq], w_sem)
            yield pltpu.make_async_copy(wk_ref.at[span], w.at[p, :, nq:nq + nk], w_sem)
            yield pltpu.make_async_copy(wv_ref.at[span], w.at[p, :, nq + nk:total_n], w_sem)

    gain_copy.wait()
    chosen = slot_ref[0]
    pltpu.make_async_copy(raw, raw, hop_send.at[0]).wait()
    for i, r in enumerate(starts):
        if i == 0:
            @pl.when(has_prev)
            def _():
                table_copy.start()
                for c in w_copies():
                    c.start()
        x = raw[0, r:r + CHUNK, :]
        for j in range(1, slots):
            x = jnp.where(jnp.full(x.shape, chosen, jnp.int32) == j, raw[j, r:r + CHUNK, :], x)
        x = x.astype(jnp.float32)
        scale = lax.rsqrt(jnp.mean(x * x, axis=-1, keepdims=True) + NORM_EPSILON)
        y = (x * scale * gain_ref[...].astype(jnp.float32)[None, :]).astype(jnp.bfloat16)
        for p in range(2 * pieces):
            mine[p, r:r + CHUNK, :] = y[:, p * half:(p + 1) * half]
    dmine[...] = jnp.zeros_like(dmine)
    doc_copy.wait()
    docs = doc_ref[0, 0:1, :]
    for i in range(1, slots):
        docs = jnp.where(jnp.full(docs.shape, chosen, jnp.int32) == i, doc_ref[0, i:i + 1, :], docs)
    dmine[0:1, 0:rows] = docs

    def edges(a):
        return a.astype(jnp.int32)

    pl.semaphore_wait(
        bar,
        edges(has_right) + edges(has_left) + edges(has_next & jnp.logical_not(greet)) + edges(has_prev & greet_prev),
    )

    @pl.when(has_prev & greet_prev)
    def _():
        pl.semaphore_signal(ready, inc=1, device_id={"section": sec - 1}, device_id_type=MESH)

    def remote(src, dst, ss, rs, target):
        return pltpu.make_async_remote_copy(
            src_ref=src, dst_ref=dst, send_sem=ss, recv_sem=rs, device_id=target, device_id_type=MESH
        )

    def sent(count, sem):
        for m in range(1, pieces + 1):
            @pl.when(count == m)
            def _():
                b = xbuf.at[0, pl.ds(0, 2 * m)]
                remote(b, b, sem, sem, {"section": sec}).wait_send()

    def whole(p):
        return pl.ds(2 * p, 2)

    def first():
        return pl.ds(2 * pieces - 2, 1)

    def second():
        return pl.ds(2 * pieces - 1, 1)

    def hop(src, c, p):
        return remote(src, xbuf.at[c, whole(p)], hop_send.at[c], recv.at[c, p], {"section": sec + 1})

    def shift(p):
        return hop(mine.at[whole(p)], me, p)

    def shift_last():
        return [
            remote(mine.at[at], xbuf.at[me, at], hop_send.at[me], rs, {"section": sec + 1})
            for at, rs in ((first(), recv.at[me, pieces - 1]), (second(), recv2.at[me]))
        ]

    def zright(src, c, p):
        return remote(src, zbuf.at[c, whole(p)], zrecv.at[c, p], zrecv.at[c, p], {"tp": me + 1})

    def zleft(src, c, p, own=False):
        return remote(
            src, zbuf.at[c, whole(p)], zleft_send if own else zrecv.at[c, p], zrecv.at[c, p], {"tp": me - 1}
        )

    def to_right(at, c, rs):
        b = xbuf.at[c, at]
        return remote(b, b, rs, rs, {"tp": me + 1})

    def to_left(at, c, rs, own=False):
        b = xbuf.at[c, at]
        return remote(b, b, left_send if own else rs, rs, {"tp": me - 1})

    def right(c, p):
        return to_right(whole(p), c, recv.at[c, p])

    def left(c, p, own=False):
        return to_left(whole(p), c, recv.at[c, p], own)

    def right_last(c):
        return [to_right(first(), c, recv.at[c, pieces - 1]), to_right(second(), c, recv2.at[c])]

    def left_last(c, own=False):
        return [to_left(first(), c, recv.at[c, pieces - 1], own), to_left(second(), c, recv2.at[c], own)]

    def each(copies, act):
        for c in copies:
            act(c)

    def pick(p, ordinary, last, act):
        @pl.when(p < pieces - 1)
        def _():
            act(ordinary())

        @pl.when(p == pieces - 1)
        def _():
            each(last(), act)

    def start(c):
        c.start()

    def wait_send(c):
        c.wait_send()

    def wait_recv(c):
        c.wait_recv()

    def dshift():
        return remote(dmine, dbuf.at[me], dshift_send, drecv.at[me], {"section": sec + 1})

    def dright(c):
        b = dbuf.at[c]
        return remote(b, b, drecv.at[c], drecv.at[c], {"tp": me + 1})

    def dleft(c, own=False):
        b = dbuf.at[c]
        return remote(b, b, dleft_send if own else drecv.at[c], drecv.at[c], {"tp": me - 1})

    def both_ways(cond_right, cond_left, go_right, go_left):
        low = 2 * me < n

        @pl.when(cond_left & low)
        def _():
            go_left()

        @pl.when(cond_right)
        def _():
            go_right()

        @pl.when(cond_left & jnp.logical_not(low))
        def _():
            go_left()

    @pl.when(has_next)
    def _():
        def own_ways():
            for p in range(pieces - 1):
                both_ways(
                    has_right & (p < early), has_left & (p < early),
                    lambda: zright(mine.at[whole(p)], me, p).start(),
                    lambda: zleft(mine.at[whole(p)], me, p, True).start(),
                )

        def hops():
            @pl.when(greet)
            def _():
                pl.semaphore_wait(ready, 1)

            dshift().start()
            for p in range(pieces - 1):
                @pl.when(p >= early)
                def _():
                    shift(p).start()

            each(shift_last(), start)
            for p in range(pieces - 1):
                @pl.when(p < early)
                def _():
                    shift(p).start()

        @pl.when(odd)
        def _():
            own_ways()
            hops()

        @pl.when(even)
        def _():
            hops()
            own_ways()

    tile = 256

    def compute(c, p, last, halves=2):
        at = pl.ds(2 * p if halves == 2 else p, halves)
        x = xbuf[c, at]
        x = jnp.concatenate([x[j] for j in range(halves)], axis=1)
        for t in range(0, total_n, tile):
            wt = w[at, :, t:t + tile].reshape(halves * half, tile)
            acc[c, :, t:t + tile] += jnp.dot(x, wt, preferred_element_type=jnp.float32)

        if last is False:
            return

        def finish():
            span = pl.ds(pl.multiple_of(c * rows, rows), rows)
            cos, sin = table[0, span, :], table[1, span, :]
            for h in range(0, nq + nk, HEAD_SIZE):
                u = acc[c, :, h:h + HEAD_SIZE]
                u = (u * cos + pltpu.roll(u, HEAD_SIZE // 2, 1) * sin).astype(jnp.bfloat16)
                if h < nq:
                    q[span, h:h + HEAD_SIZE] = u
                else:
                    k[span, h - nq:h - nq + HEAD_SIZE] = u
            v[span, :] = acc[c, :, nq + nk:total_n].astype(jnp.bfloat16)

        if last is True:
            finish()
        else:
            pl.when(last)(finish)

    heads = nk // HEAD_SIZE
    group = nq // nk
    factor = math.log2(math.e) / math.sqrt(HEAD_SIZE)

    def attend(i):
        span = pl.ds(pl.multiple_of(i * rows, rows), rows)
        lane_docs = jnp.concatenate([drow[c, 0:1, 0:rows] for c in range(n)], axis=1).astype(jnp.float32)
        i_idx = lax.broadcasted_iota(jnp.int32, (rows, total), 0) + i * rows
        j_idx = lax.broadcasted_iota(jnp.int32, (rows, total), 1)
        allowed = (j_idx <= i_idx) & (dcol[span, 0:1] == lane_docs)
        for g in range(heads):
            cols = slice(g * HEAD_SIZE, (g + 1) * HEAD_SIZE)
            qs = jnp.concatenate(
                [q[span, h * HEAD_SIZE:(h + 1) * HEAD_SIZE] for h in range(g * group, (g + 1) * group)], axis=0
            )
            scores = lax.dot_general(
                qs, k[:, cols], (((1,), (1,)), ((), ())), preferred_element_type=jnp.float32
            )
            for h in range(group):
                s_buf[g, h * rows:(h + 1) * rows, :] = jnp.where(
                    allowed, scores[h * rows:(h + 1) * rows], -1e30
                )
        for g in range(heads):
            for h in range(group):
                x = s_buf[g, h * rows:(h + 1) * rows, :]
                e = jnp.exp2((x - jnp.max(x, axis=-1, keepdims=True)) * factor)
                p_buf[g, h * rows:(h + 1) * rows, :] = e.astype(jnp.bfloat16)
        for g in range(heads):
            vg = v[:, g * HEAD_SIZE:(g + 1) * HEAD_SIZE]
            vg = jnp.concatenate([vg, jnp.ones_like(vg)], axis=1)
            both = jnp.dot(p_buf[g], vg, preferred_element_type=jnp.float32)
            both = (both[:, 0:HEAD_SIZE] / both[:, HEAD_SIZE:]).astype(jnp.bfloat16)
            for h in range(group):
                at = (g * group + h) * HEAD_SIZE
                out_ref[0, span, at:at + HEAD_SIZE] = both[h * rows:(h + 1) * rows]

    def attend_range(low, high):
        @pl.loop(low, high)
        def _(i):
            attend(i)

    def own_forward(p):
        held = (me == n - 2) & (p >= pieces - HELD) if hold else jnp.bool_(False)

        both_ways(
            has_right & jnp.logical_not(held), has_left,
            lambda: pick(p, lambda: right(me, p), lambda: right_last(me), start),
            lambda: pick(p, lambda: left(me, p, True), lambda: left_last(me, True), start),
        )

    def compute_own(p):
        @pl.when(p < early_prev)
        def _():
            shift(p).wait_recv()

        compute(me, p, p == pieces - 1)

    def weights_here():
        table_copy.wait()
        pltpu.make_async_copy(w, w, w_sem).wait()

    def keep_docs(c):
        drow[c] = dbuf[c]
        lanes = dbuf.shape[2]
        wide = jnp.broadcast_to(dbuf[c, 0:1, :].astype(jnp.float32), (lanes, lanes))
        dcol[pl.ds(pl.multiple_of(c * rows, rows), rows), :] = wide.T[0:rows, :]

    def pass_early(d, p):
        below, above = me - d, me + d

        @pl.when(below >= 0)
        def _():
            b = zbuf.at[below, whole(p)]
            zright(b, below, p).wait_recv()

            @pl.when(has_right)
            def _():
                zright(b, below, p).start()

            hop(b, below, p).start()

        @pl.when(above < n)
        def _():
            b = zbuf.at[above, whole(p)]
            zleft(b, above, p).wait_recv()

            @pl.when(has_left)
            def _():
                zleft(b, above, p).start()

            hop(b, above, p).start()

    def pass_all(d):
        if n > 1:
            @pl.loop(0, pieces - 1)
            def _(e):
                @pl.when(e < early)
                def _():
                    pass_early(d, e)

    @pl.when(has_prev)
    def _():
        acc[...] = jnp.zeros_like(acc)
        k[...] = jnp.zeros_like(k)
        v[...] = jnp.zeros_like(v)
        drow[...] = jnp.zeros_like(drow)

        dshift().wait_recv()

        @pl.when(has_right)
        def _():
            dright(me).start()

        @pl.when(has_left)
        def _():
            dleft(me, True).start()

        keep_docs(me)

        @pl.loop(early_prev, pieces)
        def _(p):
            pick(p, lambda: shift(p), shift_last, wait_recv)
            own_forward(p)

            @pl.when(p == jnp.where(even, early_prev, pieces - 1))
            def _():
                pass_all(1)

        @pl.when(at_end)
        def _():
            weights_here()

            @pl.loop(0, pieces)
            def _(p):
                compute_own(p)

        attend_range(0, jnp.where((me == 0) & (n > 1), 1, 0))

    def take_early(c):
        @pl.loop(0, pieces - 1)
        def _(p):
            @pl.when(p < early_prev)
            def _():
                hop(xbuf.at[c, whole(p)], c, p).wait_recv()
                compute(c, p, False)

    def drain():
        @pl.when(has_prev)
        def _():
            @pl.when(has_right)
            def _():
                dright(me).wait_send()
                for p in range(pieces - 1):
                    @pl.when(p >= early_prev)
                    def _():
                        right(me, p).wait_send()
                each(right_last(me), wait_send)

            @pl.when(has_left)
            def _():
                dleft(me, True).wait_send()
                sent(pieces - early_prev, left_send)

            for d in range(1, n):
                below, above = me - d, me + d

                @pl.when((below >= 0) & has_right)
                def _():
                    dright(below).wait_send()
                    for p in range(pieces - 1):
                        @pl.when(p >= early_prev)
                        def _():
                            right(below, p).wait_send()
                    each(right_last(below), wait_send)

                @pl.when((above < n) & has_left)
                def _():
                    dleft(above).wait_send()
                    for p in range(pieces - 1):
                        @pl.when(p >= early_prev)
                        def _():
                            left(above, p).wait_send()
                    each(left_last(above), wait_send)

        @pl.when(has_next)
        def _():
            dshift().wait_send()
            sent(pieces, hop_send.at[me])

            @pl.when(early > 0)
            def _():
                @pl.when(has_left)
                def _():
                    sent(early, zleft_send)

                @pl.when(has_right)
                def _():
                    for p in range(pieces - 1):
                        @pl.when(p < early)
                        def _():
                            zright(mine.at[whole(p)], me, p).wait_send()

                for d in range(1, n):
                    below, above = me - d, me + d

                    @pl.when(below >= 0)
                    def _():
                        sent(early, hop_send.at[below])

                        @pl.when(has_right)
                        def _():
                            for p in range(pieces - 1):
                                @pl.when(p < early)
                                def _():
                                    zright(zbuf.at[below, whole(p)], below, p).wait_send()

                    @pl.when(above < n)
                    def _():
                        sent(early, hop_send.at[above])

                        @pl.when(has_left)
                        def _():
                            for p in range(pieces - 1):
                                @pl.when(p < early)
                                def _():
                                    zleft(zbuf.at[above, whole(p)], above, p).wait_send()

    def take_last(c):
        for t, r in enumerate(right_last(c)):
            r.wait_recv()
            compute(c, 2 * pieces - 2 + t, t == 1, 1)

    def pass_now(d, p):
        @pl.when(jnp.where(even, (p == pieces - 1) & (d < n - 1), (p == 0) & (d > 1)))
        def _():
            pass_all(jnp.where(even, d + 1, d))

    @pl.when(has_prev & at_end)
    def _():
        drain_at = jnp.where(even & (n > 2), (n - 3) * pieces + pieces - 1, (n - 2) * pieces + 1)
        ahead = (early_prev == 1) & (n > 2)

        @pl.loop(0, (n - 1) * pieces)
        def _(i):
            d, p = i // pieces + 1, i % pieces
            c = jnp.where(me == 0, d, n - 1 - d)
            go = p >= early_prev
            if hold:
                go = go & jnp.logical_not((me == n - 1) & (d == 1) & (p >= pieces - HELD))

            pass_now(d, p)

            @pl.when(p == 0)
            def _():
                dright(c).wait_recv()
                keep_docs(c)

            @pl.when(i == drain_at)
            def _():
                drain()

            sooner = ahead & (d == n - 2) & (p == pieces - 1)
            usual = (p == pieces - 2) & jnp.logical_not(ahead & (d == n - 1))

            @pl.when((early_prev > 0) & (sooner | usual))
            def _():
                take_early(jnp.where(sooner, jnp.where(me == 0, n - 1, 0), c))

            @pl.when(go & (p < pieces - 1))
            def _():
                right(c, p).wait_recv()
                compute(c, p, False)

            @pl.when(go & (p == pieces - 1) & (i < (n - 1) * pieces - 1))
            def _():
                take_last(c)

            @pl.when((p == pieces - 1) & (me == 0) & (d < n - 1))
            def _():
                attend(d)

        @pl.when(me == 0)
        def _():
            take_last(n - 1)
            attend(n - 1)

        @pl.when(me > 0)
        def _():
            take_last(0)
            if hold:
                attend_range(0, n - 2)
                for p in range(pieces - HELD, pieces - 1):
                    @pl.when(p >= early_prev)
                    def _():
                        right(n - 2, p).wait_recv()
                        compute(n - 2, p, False)

                take_last(n - 2)
            for t in range(max(n - 2, 0), n):
                attend(t)

    @pl.when(has_prev & jnp.logical_not(at_end))
    def _():
        @pl.loop(0, (n - 1) * pieces)
        def _(i):
            d, p = i // pieces + 1, i % pieces
            below, above = me - d, me + d
            late = p >= early_prev
            final = p == pieces - 1

            pass_now(d, p)

            @pl.when((below >= 0) & (p == 0))
            def _():
                dright(below).wait_recv()
                dright(below).start()
                keep_docs(below)

            @pl.when((above < n) & (p == 0))
            def _():
                dleft(above).wait_recv()
                dleft(above).start()
                keep_docs(above)

            def forward(c):
                c.wait_recv()
                c.start()

            @pl.when(late & (below >= 0))
            def _():
                pick(p, lambda: right(below, p), lambda: right_last(below), forward)

            if hold:
                @pl.when((me == n - 2) & (d == n - 2) & final)
                def _():
                    for t in range(pieces - HELD, pieces - 1):
                        @pl.when(t >= early_prev)
                        def _():
                            right(me, t).start()
                    each(right_last(me), start)

            @pl.when(late & (above < n))
            def _():
                pick(p, lambda: left(above, p), lambda: left_last(above), forward)

            @pl.when(i == 0)
            def _():
                weights_here()

            @pl.when((p == pieces - 2) & (early_prev > 0))
            def _():
                @pl.when(below >= 0)
                def _():
                    take_early(below)

                @pl.when(above < n)
                def _():
                    take_early(above)

            @pl.when(d == min(2, n - 1))
            def _():
                compute_own(p)

            @pl.when(late & (below >= 0))
            def _():
                compute(below, p, final)

            @pl.when(late & (above < n))
            def _():
                compute(above, p, final)

        attend_range(0, n)

    @pl.when(jnp.logical_not(has_prev & at_end))
    def _():
        drain()

    @pl.when(jnp.logical_not(has_prev))
    def _():
        out_ref[...] = jnp.zeros_like(out_ref)


def in_hbm(a):
    return pltpu.with_memory_space_constraint(a, pltpu.HBM)


def per_device(stash, slot, doc_ids, norm_gain, w_query, w_key, value_weight):
    n, ns = lax.axis_size("tp"), lax.axis_size("section")
    _, slots, rows, width = stash.shape
    total = n * rows
    nq, nk = w_query.shape[1], w_key.shape[1]
    total_n = nq + nk + value_weight.shape[1]
    table = rope_tables(total)
    lanes = -(-rows // 128) * 128
    bf, f32, dma = jnp.bfloat16, jnp.float32, pltpu.SemaphoreType.DMA
    part = width // PIECES
    heads, stacked = nk // HEAD_SIZE, nq // nk * rows
    operands = (stash, doc_ids, norm_gain, jnp.asarray(table), w_query, w_key, value_weight)
    return pl.pallas_call(
        functools.partial(kernel, n, ns),
        out_shape=jax.ShapeDtypeStruct((1, total, nq), bf),
        in_specs=[pl.BlockSpec(memory_space=pltpu.SMEM)] + [ANY] * 7,
        out_specs=VMEM,
        scratch_shapes=[
            pltpu.VMEM((slots, rows, width), bf),
            pltpu.VMEM((2 * PIECES, rows, part // 2), bf),
            pltpu.VMEM((8, lanes), jnp.int32),
            pltpu.VMEM((2 * PIECES, part // 2, total_n), bf),
            pltpu.VMEM((n, 2 * PIECES, rows, part // 2), bf),
            pltpu.VMEM((n, 2 * PIECES - 2, rows, part // 2), bf),
            pltpu.VMEM((n, 8, lanes), jnp.int32),
            pltpu.VMEM((n, rows, total_n), f32),
            pltpu.VMEM((total, nq), bf),
            pltpu.VMEM((total, nk), bf),
            pltpu.VMEM((total, nk), bf),
            pltpu.VMEM((total, lanes), f32),
            pltpu.VMEM((n, 8, lanes), jnp.int32),
            pltpu.VMEM((heads, stacked, total), f32),
            pltpu.VMEM((heads, stacked, total), bf),
            dma,
            dma((max(n, rows // CHUNK),)),
            dma,
            dma((n, PIECES)),
            dma((n,)),
            dma,
            dma((n, PIECES - 1)),
            dma,
            dma,
            dma((n,)),
            dma,
            pltpu.SemaphoreType.REGULAR,
            pltpu.VMEM(doc_ids.shape, jnp.int32),
            pltpu.VMEM(norm_gain.shape, bf),
            pltpu.VMEM(table.shape, f32),
        ],
        compiler_params=pltpu.CompilerParams(
            collective_id=0, has_side_effects=True, vmem_limit_bytes=VMEM_GRANT
        ),
        cost_estimate=pl.CostEstimate(
            flops=2 * total * width * total_n, bytes_accessed=width * total_n * 2, transcendentals=0
        ),
    )(slot, *(in_hbm(a) for a in operands))


def solution(mesh):
    placed = (
        P("section", None, "tp", None),
        P("section"),
        P("section", None, "tp"),
        P(),
        P(None, "tp"),
        P(None, "tp"),
        P(None, "tp"),
    )
    return jax.shard_map(
        per_device, mesh=mesh, in_specs=placed, out_specs=P("section", None, "tp"), check_vma=False
    )
```

```python
import functools
import math

import jax
import jax.numpy as jnp
import numpy as np
from jax import lax
from jax.experimental import pallas as pl
from jax.experimental.pallas import tpu as pltpu
from jax.sharding import PartitionSpec as P

HEAD_SIZE = 128
ROPE_BASE = 500000.0
NORM_EPSILON = 1e-05
PIECES = 4
HELD = 1
CHUNK = 16
MESH = pl.DeviceIdType.MESH
VMEM_GRANT = 32 << 20
ANY = pl.BlockSpec(memory_space=pltpu.HBM)
VMEM = pl.BlockSpec(memory_space=pltpu.VMEM)


def rope_tables(length):
    half = HEAD_SIZE // 2
    freq = np.arange(half, dtype=np.float32)
    inverse = np.power(np.float32(ROPE_BASE), np.float32(-2.0) * freq / np.float32(HEAD_SIZE)).astype(np.float32)
    angles = np.arange(length, dtype=np.float32)[:, None] * inverse[None, :]
    cos, sin = np.cos(angles), np.sin(angles)
    return np.stack([
        np.concatenate([cos, cos], -1).astype(np.float32),
        np.concatenate([-sin, sin], -1).astype(np.float32),
    ])


def early_pieces(sec, ns):
    pairs = ns // 2
    count = PIECES * jnp.maximum(pairs - 1 - sec // 2, 0) // pairs if pairs else 0 * sec
    first = jnp.where((sec > 0) & (sec + 2 == ns), 1, 0)
    return jnp.where((sec % 2 == 1) & (sec + 1 < ns), count, first)


def kernel(
    n, ns,
    slot_ref, stash_ref, doc_hbm, gain_hbm, table_hbm, wq_ref, wk_ref, wv_ref,
    out_ref,
    raw, mine, dmine, w, xbuf, zbuf, dbuf, acc, q, k, v, dcol, drow, s_buf, p_buf,
    w_sem, hop_send, left_send, recv, recv2, zleft_send, zrecv,
    dshift_send, dleft_send, drecv, table_sem, ready,
    doc_ref, gain_ref, table,
):
    me = lax.axis_index("tp")
    sec = lax.axis_index("section")
    slots, rows, width = raw.shape
    pieces = PIECES
    part = width // pieces
    half = part // 2
    nq, nk = wq_ref.shape[1], wk_ref.shape[1]
    total_n = w.shape[2]
    total = n * rows
    hold = n > 2
    even, odd = sec % 2 == 0, sec % 2 == 1
    at_end = (me == 0) | (me == n - 1)
    has_right, has_left = me + 1 < n, me > 0
    has_next, has_prev = sec + 1 < ns, sec > 0
    early, early_prev = early_pieces(sec, ns), early_pieces(sec - 1, ns)
    greet, greet_prev = odd & (early >= 2), even & (early_prev >= 2)

    bar = pltpu.get_barrier_semaphore()
    for cond, target in (
        (has_right, {"tp": me + 1}),
        (has_left, {"tp": me - 1}),
        (has_next & greet, {"section": sec + 1}),
        (has_prev & jnp.logical_not(greet_prev), {"section": sec - 1}),
    ):
        @pl.when(cond)
        def _():
            pl.semaphore_signal(bar, inc=1, device_id=target, device_id_type=MESH)

    starts = range(0, rows, CHUNK)
    raw_copies = [pltpu.make_async_copy(stash_ref.at[0, :, pl.ds(r, CHUNK)], raw.at[:, pl.ds(r, CHUNK)], hop_send.at[0]) for r in starts]
    gain_copy = pltpu.make_async_copy(gain_hbm, gain_ref, left_send)
    doc_copy = pltpu.make_async_copy(doc_hbm, doc_ref, zleft_send)
    table_copy = pltpu.make_async_copy(table_hbm, table, table_sem)
    for c in raw_copies + [gain_copy, doc_copy]:
        c.start()

    def w_copies():
        for p in range(2 * pieces):
            span = pl.ds(p * half, half)
            yield pltpu.make_async_copy(wq_ref.at[span], w.at[p, :, 0:nq], w_sem)
            yield pltpu.make_async_copy(wk_ref.at[span], w.at[p, :, nq:nq + nk], w_sem)
            yield pltpu.make_async_copy(wv_ref.at[span], w.at[p, :, nq + nk:total_n], w_sem)

    gain_copy.wait()
    chosen = slot_ref[0]
    pltpu.make_async_copy(raw, raw, hop_send.at[0]).wait()
    for i, r in enumerate(starts):
        if i == 0:
            @pl.when(has_prev)
            def _():
                table_copy.start()
                for c in w_copies():
                    c.start()
        x = raw[0, r:r + CHUNK, :]
        for j in range(1, slots):
            x = jnp.where(jnp.full(x.shape, chosen, jnp.int32) == j, raw[j, r:r + CHUNK, :], x)
        x = x.astype(jnp.float32)
        scale = lax.rsqrt(jnp.mean(x * x, axis=-1, keepdims=True) + NORM_EPSILON)
        y = (x * scale * gain_ref[...].astype(jnp.float32)[None, :]).astype(jnp.bfloat16)
        for p in range(2 * pieces):
            mine[p, r:r + CHUNK, :] = y[:, p * half:(p + 1) * half]
    dmine[...] = jnp.zeros_like(dmine)
    doc_copy.wait()
    docs = doc_ref[0, 0:1, :]
    for i in range(1, slots):
        docs = jnp.where(jnp.full(docs.shape, chosen, jnp.int32) == i, doc_ref[0, i:i + 1, :], docs)
    dmine[0:1, 0:rows] = docs

    def edges(a):
        return a.astype(jnp.int32)

    pl.semaphore_wait(
        bar,
        edges(has_right) + edges(has_left) + edges(has_next & jnp.logical_not(greet)) + edges(has_prev & greet_prev),
    )

    @pl.when(has_prev & greet_prev)
    def _():
        pl.semaphore_signal(ready, inc=1, device_id={"section": sec - 1}, device_id_type=MESH)

    def remote(src, dst, ss, rs, target):
        return pltpu.make_async_remote_copy(
            src_ref=src, dst_ref=dst, send_sem=ss, recv_sem=rs, device_id=target, device_id_type=MESH
        )

    def sent(count, sem):
        for m in range(1, pieces + 1):
            @pl.when(count == m)
            def _():
                b = xbuf.at[0, pl.ds(0, 2 * m)]
                remote(b, b, sem, sem, {"section": sec}).wait_send()

    def whole(p):
        return pl.ds(2 * p, 2)

    def first():
        return pl.ds(2 * pieces - 2, 1)

    def second():
        return pl.ds(2 * pieces - 1, 1)

    def hop(src, c, p):
        return remote(src, xbuf.at[c, whole(p)], hop_send.at[c], recv.at[c, p], {"section": sec + 1})

    def shift(p):
        return hop(mine.at[whole(p)], me, p)

    def shift_last():
        return [
            remote(mine.at[at], xbuf.at[me, at], hop_send.at[me], rs, {"section": sec + 1})
            for at, rs in ((first(), recv.at[me, pieces - 1]), (second(), recv2.at[me]))
        ]

    def zright(src, c, p):
        return remote(src, zbuf.at[c, whole(p)], zrecv.at[c, p], zrecv.at[c, p], {"tp": me + 1})

    def zleft(src, c, p, own=False):
        return remote(
            src, zbuf.at[c, whole(p)], zleft_send if own else zrecv.at[c, p], zrecv.at[c, p], {"tp": me - 1}
        )

    def to_right(at, c, rs):
        b = xbuf.at[c, at]
        return remote(b, b, rs, rs, {"tp": me + 1})

    def to_left(at, c, rs, own=False):
        b = xbuf.at[c, at]
        return remote(b, b, left_send if own else rs, rs, {"tp": me - 1})

    def right(c, p):
        return to_right(whole(p), c, recv.at[c, p])

    def left(c, p, own=False):
        return to_left(whole(p), c, recv.at[c, p], own)

    def right_last(c):
        return [to_right(first(), c, recv.at[c, pieces - 1]), to_right(second(), c, recv2.at[c])]

    def left_last(c, own=False):
        return [to_left(first(), c, recv.at[c, pieces - 1], own), to_left(second(), c, recv2.at[c], own)]

    def each(copies, act):
        for c in copies:
            act(c)

    def pick(p, ordinary, last, act):
        @pl.when(p < pieces - 1)
        def _():
            act(ordinary())

        @pl.when(p == pieces - 1)
        def _():
            each(last(), act)

    def start(c):
        c.start()

    def wait_send(c):
        c.wait_send()

    def wait_recv(c):
        c.wait_recv()

    def dshift():
        return remote(dmine, dbuf.at[me], dshift_send, drecv.at[me], {"section": sec + 1})

    def dright(c):
        b = dbuf.at[c]
        return remote(b, b, drecv.at[c], drecv.at[c], {"tp": me + 1})

    def dleft(c, own=False):
        b = dbuf.at[c]
        return remote(b, b, dleft_send if own else drecv.at[c], drecv.at[c], {"tp": me - 1})

    def both_ways(cond_right, cond_left, go_right, go_left):
        low = 2 * me < n

        @pl.when(cond_left & low)
        def _():
            go_left()

        @pl.when(cond_right)
        def _():
            go_right()

        @pl.when(cond_left & jnp.logical_not(low))
        def _():
            go_left()

    @pl.when(has_next)
    def _():
        def own_ways():
            for p in range(pieces - 1):
                both_ways(
                    has_right & (p < early), has_left & (p < early),
                    lambda: zright(mine.at[whole(p)], me, p).start(),
                    lambda: zleft(mine.at[whole(p)], me, p, True).start(),
                )

        def hops():
            @pl.when(greet)
            def _():
                pl.semaphore_wait(ready, 1)

            dshift().start()
            for p in range(pieces - 1):
                @pl.when(p >= early)
                def _():
                    shift(p).start()

            each(shift_last(), start)
            for p in range(pieces - 1):
                @pl.when(p < early)
                def _():
                    shift(p).start()

        @pl.when(odd)
        def _():
            own_ways()
            hops()

        @pl.when(even)
        def _():
            hops()
            own_ways()

    tile = 256

    def compute(c, p, last, halves=2):
        at = pl.ds(2 * p if halves == 2 else p, halves)
        x = xbuf[c, at]
        x = jnp.concatenate([x[j] for j in range(halves)], axis=1)
        for t in range(0, total_n, tile):
            wt = w[at, :, t:t + tile].reshape(halves * half, tile)
            acc[c, :, t:t + tile] += jnp.dot(x, wt, preferred_element_type=jnp.float32)

        if last is False:
            return

        def finish():
            span = pl.ds(pl.multiple_of(c * rows, rows), rows)
            cos, sin = table[0, span, :], table[1, span, :]
            for h in range(0, nq + nk, HEAD_SIZE):
                u = acc[c, :, h:h + HEAD_SIZE]
                u = (u * cos + pltpu.roll(u, HEAD_SIZE // 2, 1) * sin).astype(jnp.bfloat16)
                if h < nq:
                    q[span, h:h + HEAD_SIZE] = u
                else:
                    k[span, h - nq:h - nq + HEAD_SIZE] = u
            v[span, :] = acc[c, :, nq + nk:total_n].astype(jnp.bfloat16)

        if last is True:
            finish()
        else:
            pl.when(last)(finish)

    heads = nk // HEAD_SIZE
    group = nq // nk
    factor = math.log2(math.e) / math.sqrt(HEAD_SIZE)

    def attend(i):
        span = pl.ds(pl.multiple_of(i * rows, rows), rows)
        lane_docs = jnp.concatenate([drow[c, 0:1, 0:rows] for c in range(n)], axis=1).astype(jnp.float32)
        i_idx = lax.broadcasted_iota(jnp.int32, (rows, total), 0) + i * rows
        j_idx = lax.broadcasted_iota(jnp.int32, (rows, total), 1)
        allowed = (j_idx <= i_idx) & (dcol[span, 0:1] == lane_docs)
        for g in range(heads):
            cols = slice(g * HEAD_SIZE, (g + 1) * HEAD_SIZE)
            qs = jnp.concatenate(
                [q[span, h * HEAD_SIZE:(h + 1) * HEAD_SIZE] for h in range(g * group, (g + 1) * group)], axis=0
            )
            scores = lax.dot_general(
                qs, k[:, cols], (((1,), (1,)), ((), ())), preferred_element_type=jnp.float32
            )
            for h in range(group):
                s_buf[g, h * rows:(h + 1) * rows, :] = jnp.where(
                    allowed, scores[h * rows:(h + 1) * rows], -1e30
                )
        for g in range(heads):
            for h in range(group):
                x = s_buf[g, h * rows:(h + 1) * rows, :]
                e = jnp.exp2((x - jnp.max(x, axis=-1, keepdims=True)) * factor)
                p_buf[g, h * rows:(h + 1) * rows, :] = e.astype(jnp.bfloat16)
        for g in range(heads):
            vg = v[:, g * HEAD_SIZE:(g + 1) * HEAD_SIZE]
            vg = jnp.concatenate([vg, jnp.ones_like(vg)], axis=1)
            both = jnp.dot(p_buf[g], vg, preferred_element_type=jnp.float32)
            both = (both[:, 0:HEAD_SIZE] / both[:, HEAD_SIZE:]).astype(jnp.bfloat16)
            for h in range(group):
                at = (g * group + h) * HEAD_SIZE
                out_ref[0, span, at:at + HEAD_SIZE] = both[h * rows:(h + 1) * rows]

    def attend_range(low, high):
        @pl.loop(low, high)
        def _(i):
            attend(i)

    def own_forward(p):
        held = (me == n - 2) & (p >= pieces - HELD) if hold else jnp.bool_(False)

        both_ways(
            has_right & jnp.logical_not(held), has_left,
            lambda: pick(p, lambda: right(me, p), lambda: right_last(me), start),
            lambda: pick(p, lambda: left(me, p, True), lambda: left_last(me, True), start),
        )

    def compute_own(p):
        @pl.when(p < early_prev)
        def _():
            shift(p).wait_recv()

        compute(me, p, p == pieces - 1)

    def weights_here():
        table_copy.wait()
        pltpu.make_async_copy(w, w, w_sem).wait()

    def keep_docs(c):
        drow[c] = dbuf[c]
        lanes = dbuf.shape[2]
        wide = jnp.broadcast_to(dbuf[c, 0:1, :].astype(jnp.float32), (lanes, lanes))
        dcol[pl.ds(pl.multiple_of(c * rows, rows), rows), :] = wide.T[0:rows, :]

    def pass_early(d, p):
        below, above = me - d, me + d

        @pl.when(below >= 0)
        def _():
            b = zbuf.at[below, whole(p)]
            zright(b, below, p).wait_recv()

            @pl.when(has_right)
            def _():
                zright(b, below, p).start()

            hop(b, below, p).start()

        @pl.when(above < n)
        def _():
            b = zbuf.at[above, whole(p)]
            zleft(b, above, p).wait_recv()

            @pl.when(has_left)
            def _():
                zleft(b, above, p).start()

            hop(b, above, p).start()

    def pass_all(d):
        if n > 1:
            @pl.loop(0, pieces - 1)
            def _(e):
                @pl.when(e < early)
                def _():
                    pass_early(d, e)

    @pl.when(has_prev)
    def _():
        acc[...] = jnp.zeros_like(acc)
        k[...] = jnp.zeros_like(k)
        v[...] = jnp.zeros_like(v)
        drow[...] = jnp.zeros_like(drow)

        dshift().wait_recv()

        @pl.when(has_right)
        def _():
            dright(me).start()

        @pl.when(has_left)
        def _():
            dleft(me, True).start()

        keep_docs(me)

        @pl.loop(early_prev, pieces)
        def _(p):
            pick(p, lambda: shift(p), shift_last, wait_recv)
            own_forward(p)

            @pl.when(p == jnp.where(even, early_prev, pieces - 1))
            def _():
                pass_all(1)

        @pl.when(at_end)
        def _():
            weights_here()

            @pl.loop(0, pieces)
            def _(p):
                compute_own(p)

        attend_range(0, jnp.where((me == 0) & (n > 1), 1, 0))

    def take_early(c):
        @pl.loop(0, pieces - 1)
        def _(p):
            @pl.when(p < early_prev)
            def _():
                hop(xbuf.at[c, whole(p)], c, p).wait_recv()
                compute(c, p, False)

    def drain():
        @pl.when(has_prev)
        def _():
            @pl.when(has_right)
            def _():
                dright(me).wait_send()
                for p in range(pieces - 1):
                    @pl.when(p >= early_prev)
                    def _():
                        right(me, p).wait_send()
                each(right_last(me), wait_send)

            @pl.when(has_left)
            def _():
                dleft(me, True).wait_send()
                sent(pieces - early_prev, left_send)

            for d in range(1, n):
                below, above = me - d, me + d

                @pl.when((below >= 0) & has_right)
                def _():
                    dright(below).wait_send()
                    for p in range(pieces - 1):
                        @pl.when(p >= early_prev)
                        def _():
                            right(below, p).wait_send()
                    each(right_last(below), wait_send)

                @pl.when((above < n) & has_left)
                def _():
                    dleft(above).wait_send()
                    for p in range(pieces - 1):
                        @pl.when(p >= early_prev)
                        def _():
                            left(above, p).wait_send()
                    each(left_last(above), wait_send)

        @pl.when(has_next)
        def _():
            dshift().wait_send()
            sent(pieces, hop_send.at[me])

            @pl.when(early > 0)
            def _():
                @pl.when(has_left)
                def _():
                    sent(early, zleft_send)

                @pl.when(has_right)
                def _():
                    for p in range(pieces - 1):
                        @pl.when(p < early)
                        def _():
                            zright(mine.at[whole(p)], me, p).wait_send()

                for d in range(1, n):
                    below, above = me - d, me + d

                    @pl.when(below >= 0)
                    def _():
                        sent(early, hop_send.at[below])

                        @pl.when(has_right)
                        def _():
                            for p in range(pieces - 1):
                                @pl.when(p < early)
                                def _():
                                    zright(zbuf.at[below, whole(p)], below, p).wait_send()

                    @pl.when(above < n)
                    def _():
                        sent(early, hop_send.at[above])

                        @pl.when(has_left)
                        def _():
                            for p in range(pieces - 1):
                                @pl.when(p < early)
                                def _():
                                    zleft(zbuf.at[above, whole(p)], above, p).wait_send()

    def take_last(c):
        for t, r in enumerate(right_last(c)):
            r.wait_recv()
            compute(c, 2 * pieces - 2 + t, t == 1, 1)

    def pass_now(d, p):
        @pl.when(jnp.where(even, (p == pieces - 1) & (d < n - 1), (p == 0) & (d > 1)))
        def _():
            pass_all(jnp.where(even, d + 1, d))

    @pl.when(has_prev & jnp.logical_not(at_end))
    def _():
        @pl.loop(0, (n - 1) * pieces)
        def _(i):
            d, p = i // pieces + 1, i % pieces
            below, above = me - d, me + d
            late = p >= early_prev
            final = p == pieces - 1

            pass_now(d, p)

            @pl.when((below >= 0) & (p == 0))
            def _():
                dright(below).wait_recv()
                dright(below).start()
                keep_docs(below)

            @pl.when((above < n) & (p == 0))
            def _():
                dleft(above).wait_recv()
                dleft(above).start()
                keep_docs(above)

            def forward(c):
                c.wait_recv()
                c.start()

            @pl.when(late & (below >= 0))
            def _():
                pick(p, lambda: right(below, p), lambda: right_last(below), forward)

            if hold:
                @pl.when((me == n - 2) & (d == n - 2) & final)
                def _():
                    for t in range(pieces - HELD, pieces - 1):
                        @pl.when(t >= early_prev)
                        def _():
                            right(me, t).start()
                    each(right_last(me), start)

            @pl.when(late & (above < n))
            def _():
                pick(p, lambda: left(above, p), lambda: left_last(above), forward)

            @pl.when(i == 0)
            def _():
                weights_here()

            @pl.when((p == pieces - 2) & (early_prev > 0))
            def _():
                @pl.when(below >= 0)
                def _():
                    take_early(below)

                @pl.when(above < n)
                def _():
                    take_early(above)

            @pl.when(d == min(2, n - 1))
            def _():
                compute_own(p)

            @pl.when(late & (below >= 0))
            def _():
                compute(below, p, final)

            @pl.when(late & (above < n))
            def _():
                compute(above, p, final)

        attend_range(0, n)

    @pl.when(jnp.logical_not(has_prev & at_end))
    def _():
        drain()

    @pl.when(jnp.logical_not(has_prev))
    def _():
        out_ref[...] = jnp.zeros_like(out_ref)

    @pl.when(has_prev & at_end)
    def _():
        drain_at = jnp.where(even & (n > 2), (n - 3) * pieces + pieces - 1, (n - 2) * pieces + 1)
        ahead = (early_prev == 1) & (n > 2)

        @pl.loop(0, (n - 1) * pieces)
        def _(i):
            d, p = i // pieces + 1, i % pieces
            c = jnp.where(me == 0, d, n - 1 - d)
            go = p >= early_prev
            if hold:
                go = go & jnp.logical_not((me == n - 1) & (d == 1) & (p >= pieces - HELD))

            pass_now(d, p)

            @pl.when(p == 0)
            def _():
                dright(c).wait_recv()
                keep_docs(c)

            @pl.when(i == drain_at)
            def _():
                drain()

            sooner = ahead & (d == n - 2) & (p == pieces - 1)
            usual = (p == pieces - 2) & jnp.logical_not(ahead & (d == n - 1))

            @pl.when((early_prev > 0) & (sooner | usual))
            def _():
                take_early(jnp.where(sooner, jnp.where(me == 0, n - 1, 0), c))

            @pl.when(go & (p < pieces - 1))
            def _():
                right(c, p).wait_recv()
                compute(c, p, False)

            @pl.when(go & (p == pieces - 1) & (i < (n - 1) * pieces - 1))
            def _():
                take_last(c)

            @pl.when((p == pieces - 1) & (me == 0) & (d < n - 1))
            def _():
                attend(d)

        @pl.when(me > 0)
        def _():
            take_last(0)
            if hold:
                attend_range(0, n - 2)
                for p in range(pieces - HELD, pieces - 1):
                    @pl.when(p >= early_prev)
                    def _():
                        right(n - 2, p).wait_recv()
                        compute(n - 2, p, False)

                take_last(n - 2)
            for t in range(max(n - 2, 0), n):
                attend(t)

        @pl.when(me == 0)
        def _():
            take_last(n - 1)
            attend(n - 1)


def in_hbm(a):
    return pltpu.with_memory_space_constraint(a, pltpu.HBM)


def per_device(stash, slot, doc_ids, norm_gain, w_query, w_key, value_weight):
    n, ns = lax.axis_size("tp"), lax.axis_size("section")
    _, slots, rows, width = stash.shape
    total = n * rows
    nq, nk = w_query.shape[1], w_key.shape[1]
    total_n = nq + nk + value_weight.shape[1]
    table = rope_tables(total)
    lanes = -(-rows // 128) * 128
    bf, f32, dma = jnp.bfloat16, jnp.float32, pltpu.SemaphoreType.DMA
    part = width // PIECES
    heads, stacked = nk // HEAD_SIZE, nq // nk * rows
    operands = (stash, doc_ids, norm_gain, jnp.asarray(table), w_query, w_key, value_weight)
    return pl.pallas_call(
        functools.partial(kernel, n, ns),
        out_shape=jax.ShapeDtypeStruct((1, total, nq), bf),
        in_specs=[pl.BlockSpec(memory_space=pltpu.SMEM)] + [ANY] * 7,
        out_specs=VMEM,
        scratch_shapes=[
            pltpu.VMEM((slots, rows, width), bf),
            pltpu.VMEM((2 * PIECES, rows, part // 2), bf),
            pltpu.VMEM((8, lanes), jnp.int32),
            pltpu.VMEM((2 * PIECES, part // 2, total_n), bf),
            pltpu.VMEM((n, 2 * PIECES, rows, part // 2), bf),
            pltpu.VMEM((n, 2 * PIECES - 2, rows, part // 2), bf),
            pltpu.VMEM((n, 8, lanes), jnp.int32),
            pltpu.VMEM((n, rows, total_n), f32),
            pltpu.VMEM((total, nq), bf),
            pltpu.VMEM((total, nk), bf),
            pltpu.VMEM((total, nk), bf),
            pltpu.VMEM((total, lanes), f32),
            pltpu.VMEM((n, 8, lanes), jnp.int32),
            pltpu.VMEM((heads, stacked, total), f32),
            pltpu.VMEM((heads, stacked, total), bf),
            dma,
            dma((max(n, rows // CHUNK),)),
            dma,
            dma((n, PIECES)),
            dma((n,)),
            dma,
            dma((n, PIECES - 1)),
            dma,
            dma,
            dma((n,)),
            dma,
            pltpu.SemaphoreType.REGULAR,
            pltpu.VMEM(doc_ids.shape, jnp.int32),
            pltpu.VMEM(norm_gain.shape, bf),
            pltpu.VMEM(table.shape, f32),
        ],
        compiler_params=pltpu.CompilerParams(
            collective_id=0, has_side_effects=True, vmem_limit_bytes=VMEM_GRANT
        ),
        cost_estimate=pl.CostEstimate(
            flops=2 * total * width * total_n, bytes_accessed=width * total_n * 2, transcendentals=0
        ),
    )(slot, *(in_hbm(a) for a in operands))


def solution(mesh):
    placed = (
        P("section", None, "tp", None),
        P("section"),
        P("section", None, "tp"),
        P(),
        P(None, "tp"),
        P(None, "tp"),
        P(None, "tp"),
    )
    return jax.shard_map(
        per_device, mesh=mesh, in_specs=placed, out_specs=P("section", None, "tp"), check_vma=False
    )
```

```python
import functools
import math

import jax
import jax.numpy as jnp
import numpy as np
from jax import lax
from jax.experimental import pallas as pl
from jax.experimental.pallas import tpu as pltpu
from jax.sharding import PartitionSpec as P

HEAD_SIZE = 128
ROPE_BASE = 500000.0
NORM_EPSILON = 1e-05
PIECES = 4
HELD = 1
SUBS = 32
EDGES = (0, 9, 17, 24, 32)
CHUNK = 16
MESH = pl.DeviceIdType.MESH
VMEM_GRANT = 32 << 20
ANY = pl.BlockSpec(memory_space=pltpu.HBM)
VMEM = pl.BlockSpec(memory_space=pltpu.VMEM)


def rope_tables(length):
    half = HEAD_SIZE // 2
    freq = np.arange(half, dtype=np.float32)
    inverse = np.power(np.float32(ROPE_BASE), np.float32(-2.0) * freq / np.float32(HEAD_SIZE)).astype(np.float32)
    angles = np.arange(length, dtype=np.float32)[:, None] * inverse[None, :]
    cos, sin = np.cos(angles), np.sin(angles)
    return np.stack([
        np.concatenate([cos, cos], -1).astype(np.float32),
        np.concatenate([-sin, sin], -1).astype(np.float32),
    ])


def early_pieces(sec, ns):
    pairs = ns // 2
    count = PIECES * jnp.maximum(pairs - 1 - sec // 2, 0) // pairs if pairs else 0 * sec
    first = jnp.where((sec > 0) & (sec + 2 == ns), 1, 0)
    return jnp.where((sec % 2 == 1) & (sec + 1 < ns), count, first)


def kernel(
    n, ns,
    slot_ref, stash_ref, doc_hbm, gain_hbm, table_hbm, wq_ref, wk_ref, wv_ref,
    out_ref,
    raw, mine, dmine, w, xbuf, zbuf, dbuf, acc, q, k, v, dcol, drow, s_buf, p_buf,
    w_sem, hop_send, left_send, recv, recv2, zleft_send, zrecv,
    dshift_send, dleft_send, drecv, table_sem, ready,
    doc_ref, gain_ref, table,
):
    me = lax.axis_index("tp")
    sec = lax.axis_index("section")
    slots, rows, width = raw.shape
    pieces = PIECES
    part = width // pieces
    sub = width // SUBS
    nq, nk = wq_ref.shape[1], wk_ref.shape[1]
    total_n = w.shape[1]
    total = n * rows
    hold = n > 2
    even, odd = sec % 2 == 0, sec % 2 == 1
    at_end = (me == 0) | (me == n - 1)
    has_right, has_left = me + 1 < n, me > 0
    has_next, has_prev = sec + 1 < ns, sec > 0
    early, early_prev = early_pieces(sec, ns), early_pieces(sec - 1, ns)
    greet, greet_prev = odd & (early >= 2), even & (early_prev >= 2)

    bar = pltpu.get_barrier_semaphore()
    for cond, target in (
        (has_right, {"tp": me + 1}),
        (has_left, {"tp": me - 1}),
        (has_next & greet, {"section": sec + 1}),
        (has_prev & jnp.logical_not(greet_prev), {"section": sec - 1}),
    ):
        @pl.when(cond)
        def _():
            pl.semaphore_signal(bar, inc=1, device_id=target, device_id_type=MESH)

    starts = range(0, rows, CHUNK)
    raw_copies = [pltpu.make_async_copy(stash_ref.at[0, :, pl.ds(r, CHUNK)], raw.at[:, pl.ds(r, CHUNK)], hop_send.at[0]) for r in starts]
    gain_copy = pltpu.make_async_copy(gain_hbm, gain_ref, left_send)
    doc_copy = pltpu.make_async_copy(doc_hbm, doc_ref, zleft_send)
    table_copy = pltpu.make_async_copy(table_hbm, table, table_sem)
    for c in raw_copies + [gain_copy, doc_copy]:
        c.start()

    def w_copies():
        for p in range(pieces):
            span = pl.ds(p * part, part)
            yield pltpu.make_async_copy(wq_ref.at[span], w.at[span, 0:nq], w_sem)
            yield pltpu.make_async_copy(wk_ref.at[span], w.at[span, nq:nq + nk], w_sem)
            yield pltpu.make_async_copy(wv_ref.at[span], w.at[span, nq + nk:total_n], w_sem)

    gain_copy.wait()
    chosen = slot_ref[0]
    pltpu.make_async_copy(raw, raw, hop_send.at[0]).wait()
    for i, r in enumerate(starts):
        if i == 0:
            @pl.when(has_prev)
            def _():
                table_copy.start()
                for c in w_copies():
                    c.start()
        x = raw[0, r:r + CHUNK, :]
        for j in range(1, slots):
            x = jnp.where(jnp.full(x.shape, chosen, jnp.int32) == j, raw[j, r:r + CHUNK, :], x)
        x = x.astype(jnp.float32)
        scale = lax.rsqrt(jnp.mean(x * x, axis=-1, keepdims=True) + NORM_EPSILON)
        y = (x * scale * gain_ref[...].astype(jnp.float32)[None, :]).astype(jnp.bfloat16)
        for p in range(SUBS):
            mine[p, r:r + CHUNK, :] = y[:, p * sub:(p + 1) * sub]
    dmine[...] = jnp.zeros_like(dmine)
    doc_copy.wait()
    docs = doc_ref[0, 0:1, :]
    for i in range(1, slots):
        docs = jnp.where(jnp.full(docs.shape, chosen, jnp.int32) == i, doc_ref[0, i:i + 1, :], docs)
    dmine[0:1, 0:rows] = docs

    def edges(a):
        return a.astype(jnp.int32)

    pl.semaphore_wait(
        bar,
        edges(has_right) + edges(has_left) + edges(has_next & jnp.logical_not(greet)) + edges(has_prev & greet_prev),
    )

    @pl.when(has_prev & greet_prev)
    def _():
        pl.semaphore_signal(ready, inc=1, device_id={"section": sec - 1}, device_id_type=MESH)

    def remote(src, dst, ss, rs, target):
        return pltpu.make_async_remote_copy(
            src_ref=src, dst_ref=dst, send_sem=ss, recv_sem=rs, device_id=target, device_id_type=MESH
        )

    def sent(count, sem, amounts):
        for m, amount in enumerate(amounts):
            if amount:
                @pl.when(count == m)
                def _():
                    b = xbuf.at[0, pl.ds(0, amount)]
                    remote(b, b, sem, sem, {"section": sec}).wait_send()

    def span_of(p):
        return EDGES[p], EDGES[p + 1] - EDGES[p]

    def whole(p):
        return pl.ds(*span_of(p))

    low_half = (EDGES[-2], (SUBS - EDGES[-2]) // 2)
    high_half = (EDGES[-2] + low_half[1], SUBS - EDGES[-2] - low_half[1])

    def first():
        return pl.ds(*low_half)

    def second():
        return pl.ds(*high_half)

    def by_piece(p, body):
        for q in range(pieces - 1):
            pl.when(p == q)(functools.partial(body, q))

    def hop(src, c, p):
        return remote(src, xbuf.at[c, whole(p)], hop_send.at[c], recv.at[c, p], {"section": sec + 1})

    def shift(p):
        return hop(mine.at[whole(p)], me, p)

    def shift_last():
        return [
            remote(mine.at[at], xbuf.at[me, at], hop_send.at[me], rs, {"section": sec + 1})
            for at, rs in ((first(), recv.at[me, pieces - 1]), (second(), recv2.at[me]))
        ]

    def zright(src, c, p):
        return remote(src, zbuf.at[c, whole(p)], zrecv.at[c, p], zrecv.at[c, p], {"tp": me + 1})

    def zleft(src, c, p, own=False):
        return remote(
            src, zbuf.at[c, whole(p)], zleft_send if own else zrecv.at[c, p], zrecv.at[c, p], {"tp": me - 1}
        )

    def to_right(at, c, rs):
        b = xbuf.at[c, at]
        return remote(b, b, rs, rs, {"tp": me + 1})

    def to_left(at, c, rs, own=False):
        b = xbuf.at[c, at]
        return remote(b, b, left_send if own else rs, rs, {"tp": me - 1})

    def right(c, p):
        return to_right(whole(p), c, recv.at[c, p])

    def left(c, p, own=False):
        return to_left(whole(p), c, recv.at[c, p], own)

    def right_last(c):
        return [to_right(first(), c, recv.at[c, pieces - 1]), to_right(second(), c, recv2.at[c])]

    def left_last(c, own=False):
        return [to_left(first(), c, recv.at[c, pieces - 1], own), to_left(second(), c, recv2.at[c], own)]

    def each(copies, act):
        for c in copies:
            act(c)

    def pick(p, ordinary, last, act):
        by_piece(p, lambda q: act(ordinary(q)))

        @pl.when(p == pieces - 1)
        def _():
            each(last(), act)

    def start(c):
        c.start()

    def wait_send(c):
        c.wait_send()

    def wait_recv(c):
        c.wait_recv()

    def dshift():
        return remote(dmine, dbuf.at[me], dshift_send, drecv.at[me], {"section": sec + 1})

    def dright(c):
        b = dbuf.at[c]
        return remote(b, b, drecv.at[c], drecv.at[c], {"tp": me + 1})

    def dleft(c, own=False):
        b = dbuf.at[c]
        return remote(b, b, dleft_send if own else drecv.at[c], drecv.at[c], {"tp": me - 1})

    def both_ways(cond_right, cond_left, go_right, go_left):
        low = 2 * me < n

        @pl.when(cond_left & low)
        def _():
            go_left()

        @pl.when(cond_right)
        def _():
            go_right()

        @pl.when(cond_left & jnp.logical_not(low))
        def _():
            go_left()

    @pl.when(has_next)
    def _():
        def own_ways():
            for p in range(pieces - 1):
                both_ways(
                    has_right & (p < early), has_left & (p < early),
                    lambda: zright(mine.at[whole(p)], me, p).start(),
                    lambda: zleft(mine.at[whole(p)], me, p, True).start(),
                )

        def hops():
            @pl.when(greet)
            def _():
                pl.semaphore_wait(ready, 1)

            dshift().start()
            for p in range(pieces - 1):
                @pl.when(p >= early)
                def _():
                    shift(p).start()

            each(shift_last(), start)
            for p in range(pieces - 1):
                @pl.when(p < early)
                def _():
                    shift(p).start()

        @pl.when(odd)
        def _():
            own_ways()
            hops()

        @pl.when(even)
        def _():
            hops()
            own_ways()

    tile = 256

    def compute(c, block, last):
        here, size = block
        x = xbuf[c, pl.ds(here, size)]
        x = jnp.concatenate([x[j] for j in range(size)], axis=1)
        deep = slice(here * sub, (here + size) * sub)
        for t in range(0, total_n, tile):
            acc[c, :, t:t + tile] += jnp.dot(x, w[deep, t:t + tile], preferred_element_type=jnp.float32)

        if last is False:
            return

        def finish():
            span = pl.ds(pl.multiple_of(c * rows, rows), rows)
            cos, sin = table[0, span, :], table[1, span, :]
            for h in range(0, nq + nk, HEAD_SIZE):
                u = acc[c, :, h:h + HEAD_SIZE]
                u = (u * cos + pltpu.roll(u, HEAD_SIZE // 2, 1) * sin).astype(jnp.bfloat16)
                if h < nq:
                    q[span, h:h + HEAD_SIZE] = u
                else:
                    k[span, h - nq:h - nq + HEAD_SIZE] = u
            v[span, :] = acc[c, :, nq + nk:total_n].astype(jnp.bfloat16)

        if last is True:
            finish()
        else:
            pl.when(last)(finish)

    heads = nk // HEAD_SIZE
    group = nq // nk
    factor = math.log2(math.e) / math.sqrt(HEAD_SIZE)

    def attend(i):
        span = pl.ds(pl.multiple_of(i * rows, rows), rows)
        lane_docs = jnp.concatenate([drow[c, 0:1, 0:rows] for c in range(n)], axis=1).astype(jnp.float32)
        i_idx = lax.broadcasted_iota(jnp.int32, (rows, total), 0) + i * rows
        j_idx = lax.broadcasted_iota(jnp.int32, (rows, total), 1)
        allowed = (j_idx <= i_idx) & (dcol[span, 0:1] == lane_docs)
        for g in range(heads):
            cols = slice(g * HEAD_SIZE, (g + 1) * HEAD_SIZE)
            qs = jnp.concatenate(
                [q[span, h * HEAD_SIZE:(h + 1) * HEAD_SIZE] for h in range(g * group, (g + 1) * group)], axis=0
            )
            scores = lax.dot_general(
                qs, k[:, cols], (((1,), (1,)), ((), ())), preferred_element_type=jnp.float32
            )
            for h in range(group):
                s_buf[g, h * rows:(h + 1) * rows, :] = jnp.where(
                    allowed, scores[h * rows:(h + 1) * rows], -1e30
                )
        for g in range(heads):
            for h in range(group):
                x = s_buf[g, h * rows:(h + 1) * rows, :]
                e = jnp.exp2((x - jnp.max(x, axis=-1, keepdims=True)) * factor)
                p_buf[g, h * rows:(h + 1) * rows, :] = e.astype(jnp.bfloat16)
        for g in range(heads):
            vg = v[:, g * HEAD_SIZE:(g + 1) * HEAD_SIZE]
            vg = jnp.concatenate([vg, jnp.ones_like(vg)], axis=1)
            both = jnp.dot(p_buf[g], vg, preferred_element_type=jnp.float32)
            both = (both[:, 0:HEAD_SIZE] / both[:, HEAD_SIZE:]).astype(jnp.bfloat16)
            for h in range(group):
                at = (g * group + h) * HEAD_SIZE
                out_ref[0, span, at:at + HEAD_SIZE] = both[h * rows:(h + 1) * rows]

    def attend_range(low, high):
        @pl.loop(low, high)
        def _(i):
            attend(i)

    def own_forward(p):
        held = (me == n - 2) if hold and p >= pieces - HELD else jnp.bool_(False)
        last = p == pieces - 1
        both_ways(
            has_right & jnp.logical_not(held), has_left,
            lambda: each(right_last(me) if last else [right(me, p)], start),
            lambda: each(left_last(me, True) if last else [left(me, p, True)], start),
        )

    def compute_own(p):
        if p < pieces - 1:
            @pl.when(p < early_prev)
            def _():
                shift(p).wait_recv()

        compute(me, span_of(p), p == pieces - 1)

    def weights_here():
        table_copy.wait()
        pltpu.make_async_copy(w, w, w_sem).wait()

    def keep_docs(c):
        drow[c] = dbuf[c]
        lanes = dbuf.shape[2]
        wide = jnp.broadcast_to(dbuf[c, 0:1, :].astype(jnp.float32), (lanes, lanes))
        dcol[pl.ds(pl.multiple_of(c * rows, rows), rows), :] = wide.T[0:rows, :]

    def pass_early(d, p):
        below, above = me - d, me + d

        @pl.when(below >= 0)
        def _():
            b = zbuf.at[below, whole(p)]
            zright(b, below, p).wait_recv()

            @pl.when(has_right)
            def _():
                zright(b, below, p).start()

            hop(b, below, p).start()

        @pl.when(above < n)
        def _():
            b = zbuf.at[above, whole(p)]
            zleft(b, above, p).wait_recv()

            @pl.when(has_left)
            def _():
                zleft(b, above, p).start()

            hop(b, above, p).start()

    def pass_all(d):
        if n > 1:
            for e in range(pieces - 1):
                pl.when(e < early)(functools.partial(pass_early, d, e))

    @pl.when(has_prev)
    def _():
        acc[...] = jnp.zeros_like(acc)
        k[...] = jnp.zeros_like(k)
        v[...] = jnp.zeros_like(v)
        drow[...] = jnp.zeros_like(drow)

        dshift().wait_recv()

        @pl.when(has_right)
        def _():
            dright(me).start()

        @pl.when(has_left)
        def _():
            dleft(me, True).start()

        keep_docs(me)

        def own_piece(p):
            each(shift_last() if p == pieces - 1 else [shift(p)], wait_recv)
            own_forward(p)

            @pl.when((p == early_prev) & even | (p == pieces - 1) & odd)
            def _():
                pass_all(1)

        for p in range(pieces):
            pl.when(p >= early_prev)(functools.partial(own_piece, p))

        @pl.when(at_end)
        def _():
            weights_here()

            for p in range(pieces):
                compute_own(p)

        attend_range(0, jnp.where((me == 0) & (n > 1), 1, 0))

    def take_early(c):
        for p in range(pieces - 1):
            @pl.when(p < early_prev)
            def _():
                hop(xbuf.at[c, whole(p)], c, p).wait_recv()
                compute(c, span_of(p), False)

    def drain():
        @pl.when(has_prev)
        def _():
            @pl.when(has_right)
            def _():
                dright(me).wait_send()
                for p in range(pieces - 1):
                    @pl.when(p >= early_prev)
                    def _():
                        right(me, p).wait_send()
                each(right_last(me), wait_send)

            @pl.when(has_left)
            def _():
                dleft(me, True).wait_send()
                sent(early_prev, left_send, [SUBS - e for e in EDGES[:-1]])

            for d in range(1, n):
                below, above = me - d, me + d

                @pl.when((below >= 0) & has_right)
                def _():
                    dright(below).wait_send()
                    for p in range(pieces - 1):
                        @pl.when(p >= early_prev)
                        def _():
                            right(below, p).wait_send()
                    each(right_last(below), wait_send)

                @pl.when((above < n) & has_left)
                def _():
                    dleft(above).wait_send()
                    for p in range(pieces - 1):
                        @pl.when(p >= early_prev)
                        def _():
                            left(above, p).wait_send()
                    each(left_last(above), wait_send)

        @pl.when(has_next)
        def _():
            dshift().wait_send()
            sent(0, hop_send.at[me], [SUBS])

            @pl.when(early > 0)
            def _():
                @pl.when(has_left)
                def _():
                    sent(early, zleft_send, EDGES[:-1])

                @pl.when(has_right)
                def _():
                    for p in range(pieces - 1):
                        @pl.when(p < early)
                        def _():
                            zright(mine.at[whole(p)], me, p).wait_send()

                for d in range(1, n):
                    below, above = me - d, me + d

                    @pl.when(below >= 0)
                    def _():
                        sent(early, hop_send.at[below], EDGES[:-1])

                        @pl.when(has_right)
                        def _():
                            for p in range(pieces - 1):
                                @pl.when(p < early)
                                def _():
                                    zright(zbuf.at[below, whole(p)], below, p).wait_send()

                    @pl.when(above < n)
                    def _():
                        sent(early, hop_send.at[above], EDGES[:-1])

                        @pl.when(has_left)
                        def _():
                            for p in range(pieces - 1):
                                @pl.when(p < early)
                                def _():
                                    zleft(zbuf.at[above, whole(p)], above, p).wait_send()

    def take_last(c):
        for t, r in enumerate(right_last(c)):
            r.wait_recv()
            compute(c, (low_half, high_half)[t], t == 1)

    def pass_now(d, p):
        @pl.when(jnp.where(even, (p == pieces - 1) & (d < n - 1), (p == 0) & (d > 1)))
        def _():
            pass_all(jnp.where(even, d + 1, d))

    @pl.when(has_prev & jnp.logical_not(at_end))
    def _():
        @pl.loop(0, (n - 1) * pieces)
        def _(i):
            d, p = i // pieces + 1, i % pieces
            below, above = me - d, me + d
            late = p >= early_prev
            final = p == pieces - 1

            pass_now(d, p)

            @pl.when((below >= 0) & (p == 0))
            def _():
                dright(below).wait_recv()
                dright(below).start()
                keep_docs(below)

            @pl.when((above < n) & (p == 0))
            def _():
                dleft(above).wait_recv()
                dleft(above).start()
                keep_docs(above)

            def forward(c):
                c.wait_recv()
                c.start()

            @pl.when(late & (below >= 0))
            def _():
                pick(p, lambda q: right(below, q), lambda: right_last(below), forward)

            if hold:
                @pl.when((me == n - 2) & (d == n - 2) & final)
                def _():
                    for t in range(pieces - HELD, pieces - 1):
                        @pl.when(t >= early_prev)
                        def _():
                            right(me, t).start()
                    each(right_last(me), start)

            @pl.when(late & (above < n))
            def _():
                pick(p, lambda q: left(above, q), lambda: left_last(above), forward)

            @pl.when(i == 0)
            def _():
                weights_here()

            @pl.when((p == pieces - 2) & (early_prev > 0))
            def _():
                @pl.loop(0, 2)
                def _(j):
                    c = jnp.where(j == 0, below, above)

                    @pl.when((c >= 0) & (c < n))
                    def _():
                        take_early(c)

            def middle_piece(q):
                @pl.loop(0, 3)
                def _(j):
                    c = jnp.where(j == 0, me, jnp.where(j == 1, below, above))
                    inside = (c >= 0) & (c < n)
                    own = (j == 0) & (d == min(2, n - 1))

                    if q < pieces - 1:
                        @pl.when(own & (q < early_prev))
                        def _():
                            shift(q).wait_recv()

                    @pl.when(own | (j > 0) & late & inside)
                    def _():
                        compute(c, span_of(q), q == pieces - 1)

            for q in range(pieces):
                pl.when(p == q)(functools.partial(middle_piece, q))

        attend_range(0, n)

    @pl.when(jnp.logical_not(has_prev & at_end))
    def _():
        drain()

    @pl.when(jnp.logical_not(has_prev))
    def _():
        out_ref[...] = jnp.zeros_like(out_ref)

    @pl.when(has_prev & at_end)
    def _():
        drain_at = jnp.where(even & (n > 2), (n - 3) * pieces + pieces - 1, (n - 2) * pieces + 1)
        ahead = (early_prev == 1) & (n > 2)

        @pl.loop(0, (n - 1) * pieces)
        def _(i):
            d, p = i // pieces + 1, i % pieces
            c = jnp.where(me == 0, d, n - 1 - d)
            go = p >= early_prev
            if hold:
                go = go & jnp.logical_not((me == n - 1) & (d == 1) & (p >= pieces - HELD))

            pass_now(d, p)

            @pl.when(p == 0)
            def _():
                dright(c).wait_recv()
                keep_docs(c)

            @pl.when(i == drain_at)
            def _():
                drain()

            sooner = ahead & (d == n - 2) & (p == pieces - 1)
            usual = (p == pieces - 2) & jnp.logical_not(ahead & (d == n - 1))

            @pl.when((early_prev > 0) & (sooner | usual))
            def _():
                take_early(jnp.where(sooner, jnp.where(me == 0, n - 1, 0), c))

            def end_piece(q):
                right(c, q).wait_recv()
                compute(c, span_of(q), False)

            @pl.when(go)
            def _():
                by_piece(p, end_piece)

            @pl.when(go & (p == pieces - 1) & ((i < (n - 1) * pieces - 1) | (me > 0)))
            def _():
                take_last(c)

            @pl.when((p == pieces - 1) & (me == 0) & (d < n - 1))
            def _():
                attend(d)

        @pl.when(me > 0)
        def _():
            if hold:
                attend_range(0, n - 2)
                for p in range(pieces - HELD, pieces - 1):
                    @pl.when(p >= early_prev)
                    def _():
                        right(n - 2, p).wait_recv()
                        compute(n - 2, span_of(p), False)

                take_last(n - 2)
            for t in range(max(n - 2, 0), n):
                attend(t)

        @pl.when(me == 0)
        def _():
            take_last(n - 1)
            attend(n - 1)


def in_hbm(a):
    return pltpu.with_memory_space_constraint(a, pltpu.HBM)


def per_device(stash, slot, doc_ids, norm_gain, w_query, w_key, value_weight):
    n, ns = lax.axis_size("tp"), lax.axis_size("section")
    _, slots, rows, width = stash.shape
    total = n * rows
    nq, nk = w_query.shape[1], w_key.shape[1]
    total_n = nq + nk + value_weight.shape[1]
    table = rope_tables(total)
    lanes = -(-rows // 128) * 128
    bf, f32, dma = jnp.bfloat16, jnp.float32, pltpu.SemaphoreType.DMA
    heads, stacked = nk // HEAD_SIZE, nq // nk * rows
    operands = (stash, doc_ids, norm_gain, jnp.asarray(table), w_query, w_key, value_weight)
    return pl.pallas_call(
        functools.partial(kernel, n, ns),
        out_shape=jax.ShapeDtypeStruct((1, total, nq), bf),
        in_specs=[pl.BlockSpec(memory_space=pltpu.SMEM)] + [ANY] * 7,
        out_specs=VMEM,
        scratch_shapes=[
            pltpu.VMEM((slots, rows, width), bf),
            pltpu.VMEM((SUBS, rows, width // SUBS), bf),
            pltpu.VMEM((8, lanes), jnp.int32),
            pltpu.VMEM((width, total_n), bf),
            pltpu.VMEM((n, SUBS, rows, width // SUBS), bf),
            pltpu.VMEM((n, EDGES[-2], rows, width // SUBS), bf),
            pltpu.VMEM((n, 8, lanes), jnp.int32),
            pltpu.VMEM((n, rows, total_n), f32),
            pltpu.VMEM((total, nq), bf),
            pltpu.VMEM((total, nk), bf),
            pltpu.VMEM((total, nk), bf),
            pltpu.VMEM((total, lanes), f32),
            pltpu.VMEM((n, 8, lanes), jnp.int32),
            pltpu.VMEM((heads, stacked, total), f32),
            pltpu.VMEM((heads, stacked, total), bf),
            dma,
            dma((max(n, rows // CHUNK),)),
            dma,
            dma((n, PIECES)),
            dma((n,)),
            dma,
            dma((n, PIECES - 1)),
            dma,
            dma,
            dma((n,)),
            dma,
            pltpu.SemaphoreType.REGULAR,
            pltpu.VMEM(doc_ids.shape, jnp.int32),
            pltpu.VMEM(norm_gain.shape, bf),
            pltpu.VMEM(table.shape, f32),
        ],
        compiler_params=pltpu.CompilerParams(
            collective_id=0, has_side_effects=True, vmem_limit_bytes=VMEM_GRANT
        ),
        cost_estimate=pl.CostEstimate(
            flops=2 * total * width * total_n, bytes_accessed=width * total_n * 2, transcendentals=0
        ),
    )(slot, *(in_hbm(a) for a in operands))


def solution(mesh):
    placed = (
        P("section", None, "tp", None),
        P("section"),
        P("section", None, "tp"),
        P(),
        P(None, "tp"),
        P(None, "tp"),
        P(None, "tp"),
    )
    return jax.shard_map(
        per_device, mesh=mesh, in_specs=placed, out_specs=P("section", None, "tp"), check_vma=False
    )
```

```python
import functools
import math

import jax
import jax.numpy as jnp
import numpy as np
from jax import lax
from jax.experimental import pallas as pl
from jax.experimental.pallas import tpu as pltpu
from jax.sharding import PartitionSpec as P

HEAD_SIZE = 128
ROPE_BASE = 500000.0
NORM_EPSILON = 1e-05
PIECES = 4
HELD = 1
SUBS = 32
EDGES = (0, 9, 17, 24, 32)
CHUNK = 16
MESH = pl.DeviceIdType.MESH
VMEM_GRANT = 32 << 20
ANY = pl.BlockSpec(memory_space=pltpu.HBM)
VMEM = pl.BlockSpec(memory_space=pltpu.VMEM)


def rope_tables(length):
    half = HEAD_SIZE // 2
    freq = np.arange(half, dtype=np.float32)
    inverse = np.power(np.float32(ROPE_BASE), np.float32(-2.0) * freq / np.float32(HEAD_SIZE)).astype(np.float32)
    angles = np.arange(length, dtype=np.float32)[:, None] * inverse[None, :]
    cos, sin = np.cos(angles), np.sin(angles)
    return np.stack([
        np.concatenate([cos, cos], -1).astype(np.float32),
        np.concatenate([-sin, sin], -1).astype(np.float32),
    ])


def early_pieces(sec, ns):
    pairs = ns // 2
    count = PIECES * jnp.maximum(pairs - 1 - sec // 2, 0) // pairs if pairs else 0 * sec
    first = jnp.where((sec > 0) & (sec + 2 == ns), 1, 0)
    return jnp.where((sec % 2 == 1) & (sec + 1 < ns), count, first)


def kernel(
    n, ns,
    slot_ref, stash_ref, doc_hbm, gain_hbm, table_hbm, wq_ref, wk_ref, wv_ref,
    out_ref,
    raw, mine, dmine, w, xbuf, zbuf, dbuf, acc, q, k, v, dcol, drow, s_buf, p_buf,
    w_sem, hop_send, left_send, recv, recv2, zleft_send, zrecv,
    dshift_send, dleft_send, drecv, table_sem, ready,
    doc_ref, gain_ref, table,
):
    me = lax.axis_index("tp")
    sec = lax.axis_index("section")
    slots, rows, width = raw.shape
    pieces = PIECES
    part = width // pieces
    sub = width // SUBS
    nq, nk = wq_ref.shape[1], wk_ref.shape[1]
    total_n = w.shape[1]
    total = n * rows
    hold = n > 2
    even, odd = sec % 2 == 0, sec % 2 == 1
    at_end = (me == 0) | (me == n - 1)
    has_right, has_left = me + 1 < n, me > 0
    has_next, has_prev = sec + 1 < ns, sec > 0
    early, early_prev = early_pieces(sec, ns), early_pieces(sec - 1, ns)
    greet, greet_prev = odd & (early >= 2), even & (early_prev >= 2)

    bar = pltpu.get_barrier_semaphore()
    for cond, target in (
        (has_right, {"tp": me + 1}),
        (has_left, {"tp": me - 1}),
        (has_next & greet, {"section": sec + 1}),
        (has_prev & jnp.logical_not(greet_prev), {"section": sec - 1}),
    ):
        @pl.when(cond)
        def _():
            pl.semaphore_signal(bar, inc=1, device_id=target, device_id_type=MESH)

    starts = range(0, rows, CHUNK)
    raw_copies = [pltpu.make_async_copy(stash_ref.at[0, :, pl.ds(r, CHUNK)], raw.at[:, pl.ds(r, CHUNK)], hop_send.at[0]) for r in starts]
    gain_copy = pltpu.make_async_copy(gain_hbm, gain_ref, left_send)
    doc_copy = pltpu.make_async_copy(doc_hbm, doc_ref, zleft_send)
    table_copy = pltpu.make_async_copy(table_hbm, table, table_sem)
    for c in raw_copies + [gain_copy, doc_copy]:
        c.start()

    def w_copies():
        for p in range(pieces):
            span = pl.ds(p * part, part)
            yield pltpu.make_async_copy(wq_ref.at[span], w.at[span, 0:nq], w_sem)
            yield pltpu.make_async_copy(wk_ref.at[span], w.at[span, nq:nq + nk], w_sem)
            yield pltpu.make_async_copy(wv_ref.at[span], w.at[span, nq + nk:total_n], w_sem)

    gain_copy.wait()
    chosen = slot_ref[0]
    pltpu.make_async_copy(raw, raw, hop_send.at[0]).wait()
    for i, r in enumerate(starts):
        x = raw[0, r:r + CHUNK, :]
        for j in range(1, slots):
            x = jnp.where(jnp.full(x.shape, chosen, jnp.int32) == j, raw[j, r:r + CHUNK, :], x)
        x = x.astype(jnp.float32)
        scale = lax.rsqrt(jnp.mean(x * x, axis=-1, keepdims=True) + NORM_EPSILON)
        y = (x * scale * gain_ref[...].astype(jnp.float32)[None, :]).astype(jnp.bfloat16)
        for p in range(SUBS):
            mine[p, r:r + CHUNK, :] = y[:, p * sub:(p + 1) * sub]
    dmine[...] = jnp.zeros_like(dmine)
    doc_copy.wait()
    docs = doc_ref[0, 0:1, :]
    for i in range(1, slots):
        docs = jnp.where(jnp.full(docs.shape, chosen, jnp.int32) == i, doc_ref[0, i:i + 1, :], docs)
    dmine[0:1, 0:rows] = docs

    def edges(a):
        return a.astype(jnp.int32)

    pl.semaphore_wait(
        bar,
        edges(has_right) + edges(has_left) + edges(has_next & jnp.logical_not(greet)) + edges(has_prev & greet_prev),
    )

    @pl.when(has_prev & greet_prev)
    def _():
        pl.semaphore_signal(ready, inc=1, device_id={"section": sec - 1}, device_id_type=MESH)

    def remote(src, dst, ss, rs, target):
        return pltpu.make_async_remote_copy(
            src_ref=src, dst_ref=dst, send_sem=ss, recv_sem=rs, device_id=target, device_id_type=MESH
        )

    def sent(count, sem, amounts):
        for m, amount in enumerate(amounts):
            if amount:
                @pl.when(count == m)
                def _():
                    b = xbuf.at[0, pl.ds(0, amount)]
                    remote(b, b, sem, sem, {"section": sec}).wait_send()

    def span_of(p):
        return EDGES[p], EDGES[p + 1] - EDGES[p]

    def whole(p):
        return pl.ds(*span_of(p))

    low_half = (EDGES[-2], (SUBS - EDGES[-2]) // 2)
    high_half = (EDGES[-2] + low_half[1], SUBS - EDGES[-2] - low_half[1])

    def first():
        return pl.ds(*low_half)

    def second():
        return pl.ds(*high_half)

    def by_piece(p, body):
        for q in range(pieces - 1):
            pl.when(p == q)(functools.partial(body, q))

    def hop(src, c, p):
        return remote(src, xbuf.at[c, whole(p)], hop_send.at[c], recv.at[c, p], {"section": sec + 1})

    def shift(p):
        return hop(mine.at[whole(p)], me, p)

    def shift_last():
        return [
            remote(mine.at[at], xbuf.at[me, at], hop_send.at[me], rs, {"section": sec + 1})
            for at, rs in ((first(), recv.at[me, pieces - 1]), (second(), recv2.at[me]))
        ]

    def zright(src, c, p):
        return remote(src, zbuf.at[c, whole(p)], zrecv.at[c, p], zrecv.at[c, p], {"tp": me + 1})

    def zleft(src, c, p, own=False):
        return remote(
            src, zbuf.at[c, whole(p)], zleft_send if own else zrecv.at[c, p], zrecv.at[c, p], {"tp": me - 1}
        )

    def to_right(at, c, rs):
        b = xbuf.at[c, at]
        return remote(b, b, rs, rs, {"tp": me + 1})

    def to_left(at, c, rs, own=False):
        b = xbuf.at[c, at]
        return remote(b, b, left_send if own else rs, rs, {"tp": me - 1})

    def right(c, p):
        return to_right(whole(p), c, recv.at[c, p])

    def left(c, p, own=False):
        return to_left(whole(p), c, recv.at[c, p], own)

    def right_last(c):
        return [to_right(first(), c, recv.at[c, pieces - 1]), to_right(second(), c, recv2.at[c])]

    def left_last(c, own=False):
        return [to_left(first(), c, recv.at[c, pieces - 1], own), to_left(second(), c, recv2.at[c], own)]

    def each(copies, act):
        for c in copies:
            act(c)

    def pick(p, ordinary, last, act):
        by_piece(p, lambda q: act(ordinary(q)))

        @pl.when(p == pieces - 1)
        def _():
            each(last(), act)

    def start(c):
        c.start()

    def wait_send(c):
        c.wait_send()

    def wait_recv(c):
        c.wait_recv()

    def dshift():
        return remote(dmine, dbuf.at[me], dshift_send, drecv.at[me], {"section": sec + 1})

    def dright(c):
        b = dbuf.at[c]
        return remote(b, b, drecv.at[c], drecv.at[c], {"tp": me + 1})

    def dleft(c, own=False):
        b = dbuf.at[c]
        return remote(b, b, dleft_send if own else drecv.at[c], drecv.at[c], {"tp": me - 1})

    def both_ways(cond_right, cond_left, go_right, go_left):
        low = 2 * me < n

        @pl.when(cond_left & low)
        def _():
            go_left()

        @pl.when(cond_right)
        def _():
            go_right()

        @pl.when(cond_left & jnp.logical_not(low))
        def _():
            go_left()

    @pl.when(has_next)
    def _():
        def own_ways():
            for p in range(pieces - 1):
                both_ways(
                    has_right & (p < early), has_left & (p < early),
                    lambda: zright(mine.at[whole(p)], me, p).start(),
                    lambda: zleft(mine.at[whole(p)], me, p, True).start(),
                )

        def hops():
            @pl.when(greet)
            def _():
                pl.semaphore_wait(ready, 1)

            dshift().start()
            for p in range(pieces - 1):
                @pl.when(p >= early)
                def _():
                    shift(p).start()

            each(shift_last(), start)
            for p in range(pieces - 1):
                @pl.when(p < early)
                def _():
                    shift(p).start()

        @pl.when(odd)
        def _():
            own_ways()
            hops()

        @pl.when(even)
        def _():
            hops()
            own_ways()

    @pl.when(has_prev)
    def _():
        table_copy.start()
        for c in w_copies():
            c.start()

    tile = 256

    def compute(c, block, last):
        here, size = block
        x = xbuf[c, pl.ds(here, size)]
        x = jnp.concatenate([x[j] for j in range(size)], axis=1)
        deep = slice(here * sub, (here + size) * sub)
        for t in range(0, total_n, tile):
            acc[c, :, t:t + tile] += jnp.dot(x, w[deep, t:t + tile], preferred_element_type=jnp.float32)

        if last is False:
            return

        def finish():
            span = pl.ds(pl.multiple_of(c * rows, rows), rows)
            cos, sin = table[0, span, :], table[1, span, :]
            for h in range(0, nq + nk, HEAD_SIZE):
                u = acc[c, :, h:h + HEAD_SIZE]
                u = (u * cos + pltpu.roll(u, HEAD_SIZE // 2, 1) * sin).astype(jnp.bfloat16)
                if h < nq:
                    q[span, h:h + HEAD_SIZE] = u
                else:
                    k[span, h - nq:h - nq + HEAD_SIZE] = u
            v[span, :] = acc[c, :, nq + nk:total_n].astype(jnp.bfloat16)

        if last is True:
            finish()
        else:
            pl.when(last)(finish)

    heads = nk // HEAD_SIZE
    group = nq // nk
    factor = math.log2(math.e) / math.sqrt(HEAD_SIZE)

    def attend(i):
        span = pl.ds(pl.multiple_of(i * rows, rows), rows)
        lane_docs = jnp.concatenate([drow[c, 0:1, 0:rows] for c in range(n)], axis=1).astype(jnp.float32)
        i_idx = lax.broadcasted_iota(jnp.int32, (rows, total), 0) + i * rows
        j_idx = lax.broadcasted_iota(jnp.int32, (rows, total), 1)
        allowed = (j_idx <= i_idx) & (dcol[span, 0:1] == lane_docs)
        for g in range(heads):
            cols = slice(g * HEAD_SIZE, (g + 1) * HEAD_SIZE)
            qs = jnp.concatenate(
                [q[span, h * HEAD_SIZE:(h + 1) * HEAD_SIZE] for h in range(g * group, (g + 1) * group)], axis=0
            )
            scores = lax.dot_general(
                qs, k[:, cols], (((1,), (1,)), ((), ())), preferred_element_type=jnp.float32
            )
            for h in range(group):
                s_buf[g, h * rows:(h + 1) * rows, :] = jnp.where(
                    allowed, scores[h * rows:(h + 1) * rows], -1e30
                )
        for g in range(heads):
            for h in range(group):
                x = s_buf[g, h * rows:(h + 1) * rows, :]
                e = jnp.exp2((x - jnp.max(x, axis=-1, keepdims=True)) * factor)
                p_buf[g, h * rows:(h + 1) * rows, :] = e.astype(jnp.bfloat16)
        for g in range(heads):
            vg = v[:, g * HEAD_SIZE:(g + 1) * HEAD_SIZE]
            vg = jnp.concatenate([vg, jnp.ones_like(vg)], axis=1)
            both = jnp.dot(p_buf[g], vg, preferred_element_type=jnp.float32)
            both = (both[:, 0:HEAD_SIZE] / both[:, HEAD_SIZE:]).astype(jnp.bfloat16)
            for h in range(group):
                at = (g * group + h) * HEAD_SIZE
                out_ref[0, span, at:at + HEAD_SIZE] = both[h * rows:(h + 1) * rows]

    def attend_range(low, high):
        @pl.loop(low, high)
        def _(i):
            attend(i)

    def own_forward(p):
        held = (me == n - 2) if hold and p >= pieces - HELD else jnp.bool_(False)
        last = p == pieces - 1
        both_ways(
            has_right & jnp.logical_not(held), has_left,
            lambda: each(right_last(me) if last else [right(me, p)], start),
            lambda: each(left_last(me, True) if last else [left(me, p, True)], start),
        )

    def compute_own(p):
        if p < pieces - 1:
            @pl.when(p < early_prev)
            def _():
                shift(p).wait_recv()

        compute(me, span_of(p), p == pieces - 1)

    def weights_here():
        table_copy.wait()
        pltpu.make_async_copy(w, w, w_sem).wait()

    def keep_docs(c):
        drow[c] = dbuf[c]
        lanes = dbuf.shape[2]
        wide = jnp.broadcast_to(dbuf[c, 0:1, :].astype(jnp.float32), (lanes, lanes))
        dcol[pl.ds(pl.multiple_of(c * rows, rows), rows), :] = wide.T[0:rows, :]

    def pass_early(d, p):
        below, above = me - d, me + d

        @pl.when(below >= 0)
        def _():
            b = zbuf.at[below, whole(p)]
            zright(b, below, p).wait_recv()

            @pl.when(has_right)
            def _():
                zright(b, below, p).start()

            hop(b, below, p).start()

        @pl.when(above < n)
        def _():
            b = zbuf.at[above, whole(p)]
            zleft(b, above, p).wait_recv()

            @pl.when(has_left)
            def _():
                zleft(b, above, p).start()

            hop(b, above, p).start()

    def pass_all(d):
        if n > 1:
            for e in range(pieces - 1):
                pl.when(e < early)(functools.partial(pass_early, d, e))

    @pl.when(has_prev)
    def _():
        acc[...] = jnp.zeros_like(acc)
        k[...] = jnp.zeros_like(k)
        v[...] = jnp.zeros_like(v)
        drow[...] = jnp.zeros_like(drow)

        dshift().wait_recv()

        @pl.when(has_right)
        def _():
            dright(me).start()

        @pl.when(has_left)
        def _():
            dleft(me, True).start()

        keep_docs(me)

        def own_piece(p):
            each(shift_last() if p == pieces - 1 else [shift(p)], wait_recv)
            own_forward(p)

            @pl.when((p == early_prev) & even | (p == pieces - 1) & odd)
            def _():
                pass_all(1)

        for p in range(pieces):
            pl.when(p >= early_prev)(functools.partial(own_piece, p))

        @pl.when(at_end)
        def _():
            weights_here()

            for p in range(pieces):
                compute_own(p)

        attend_range(0, jnp.where((me == 0) & (n > 1), 1, 0))

    def take_early(c):
        for p in range(pieces - 1):
            @pl.when(p < early_prev)
            def _():
                hop(xbuf.at[c, whole(p)], c, p).wait_recv()
                compute(c, span_of(p), False)

    def drain():
        @pl.when(has_prev)
        def _():
            @pl.when(has_right)
            def _():
                dright(me).wait_send()
                for p in range(pieces - 1):
                    @pl.when(p >= early_prev)
                    def _():
                        right(me, p).wait_send()
                each(right_last(me), wait_send)

            @pl.when(has_left)
            def _():
                dleft(me, True).wait_send()
                sent(early_prev, left_send, [SUBS - e for e in EDGES[:-1]])

            for d in range(1, n):
                below, above = me - d, me + d

                @pl.when((below >= 0) & has_right)
                def _():
                    dright(below).wait_send()
                    for p in range(pieces - 1):
                        @pl.when(p >= early_prev)
                        def _():
                            right(below, p).wait_send()
                    each(right_last(below), wait_send)

                @pl.when((above < n) & has_left)
                def _():
                    dleft(above).wait_send()
                    for p in range(pieces - 1):
                        @pl.when(p >= early_prev)
                        def _():
                            left(above, p).wait_send()
                    each(left_last(above), wait_send)

        @pl.when(has_next)
        def _():
            dshift().wait_send()
            sent(0, hop_send.at[me], [SUBS])

            @pl.when(early > 0)
            def _():
                @pl.when(has_left)
                def _():
                    sent(early, zleft_send, EDGES[:-1])

                @pl.when(has_right)
                def _():
                    for p in range(pieces - 1):
                        @pl.when(p < early)
                        def _():
                            zright(mine.at[whole(p)], me, p).wait_send()

                for d in range(1, n):
                    below, above = me - d, me + d

                    @pl.when(below >= 0)
                    def _():
                        sent(early, hop_send.at[below], EDGES[:-1])

                        @pl.when(has_right)
                        def _():
                            for p in range(pieces - 1):
                                @pl.when(p < early)
                                def _():
                                    zright(zbuf.at[below, whole(p)], below, p).wait_send()

                    @pl.when(above < n)
                    def _():
                        sent(early, hop_send.at[above], EDGES[:-1])

                        @pl.when(has_left)
                        def _():
                            for p in range(pieces - 1):
                                @pl.when(p < early)
                                def _():
                                    zleft(zbuf.at[above, whole(p)], above, p).wait_send()

    def take_last(c):
        for t, r in enumerate(right_last(c)):
            r.wait_recv()
            compute(c, (low_half, high_half)[t], t == 1)

    def pass_now(d, p):
        @pl.when(jnp.where(even, (p == pieces - 1) & (d < n - 1), (p == 0) & (d > 1)))
        def _():
            pass_all(jnp.where(even, d + 1, d))

    @pl.when(has_prev & jnp.logical_not(at_end))
    def _():
        @pl.loop(0, (n - 1) * pieces)
        def _(i):
            d, p = i // pieces + 1, i % pieces
            below, above = me - d, me + d
            late = p >= early_prev
            final = p == pieces - 1

            pass_now(d, p)

            @pl.when((below >= 0) & (p == 0))
            def _():
                dright(below).wait_recv()
                dright(below).start()
                keep_docs(below)

            @pl.when((above < n) & (p == 0))
            def _():
                dleft(above).wait_recv()
                dleft(above).start()
                keep_docs(above)

            def forward(c):
                c.wait_recv()
                c.start()

            @pl.when(late & (below >= 0))
            def _():
                pick(p, lambda q: right(below, q), lambda: right_last(below), forward)

            if hold:
                @pl.when((me == n - 2) & (d == n - 2) & final)
                def _():
                    for t in range(pieces - HELD, pieces - 1):
                        @pl.when(t >= early_prev)
                        def _():
                            right(me, t).start()
                    each(right_last(me), start)

            @pl.when(late & (above < n))
            def _():
                pick(p, lambda q: left(above, q), lambda: left_last(above), forward)

            @pl.when(i == 0)
            def _():
                weights_here()

            @pl.when((p == pieces - 2) & (early_prev > 0))
            def _():
                @pl.loop(0, 2)
                def _(j):
                    c = jnp.where(j == 0, below, above)

                    @pl.when((c >= 0) & (c < n))
                    def _():
                        take_early(c)

            def middle_piece(q):
                @pl.loop(0, 3)
                def _(j):
                    c = jnp.where(j == 0, me, jnp.where(j == 1, below, above))
                    inside = (c >= 0) & (c < n)
                    own = (j == 0) & (d == min(2, n - 1))

                    if q < pieces - 1:
                        @pl.when(own & (q < early_prev))
                        def _():
                            shift(q).wait_recv()

                    @pl.when(own | (j > 0) & late & inside)
                    def _():
                        compute(c, span_of(q), q == pieces - 1)

            for q in range(pieces):
                pl.when(p == q)(functools.partial(middle_piece, q))

        attend_range(0, n)

    @pl.when(jnp.logical_not(has_prev & at_end))
    def _():
        drain()

    @pl.when(jnp.logical_not(has_prev))
    def _():
        out_ref[...] = jnp.zeros_like(out_ref)

    @pl.when(has_prev & at_end)
    def _():
        drain_at = jnp.where(even & (n > 2), (n - 3) * pieces + pieces - 1, (n - 2) * pieces + 1)
        ahead = (early_prev == 1) & (n > 2)

        @pl.loop(0, (n - 1) * pieces)
        def _(i):
            d, p = i // pieces + 1, i % pieces
            c = jnp.where(me == 0, d, n - 1 - d)
            go = p >= early_prev
            if hold:
                go = go & jnp.logical_not((me == n - 1) & (d == 1) & (p >= pieces - HELD))

            pass_now(d, p)

            @pl.when(p == 0)
            def _():
                dright(c).wait_recv()
                keep_docs(c)

            @pl.when(i == drain_at)
            def _():
                drain()

            sooner = ahead & (d == n - 2) & (p == pieces - 1)
            usual = (p == pieces - 2) & jnp.logical_not(ahead & (d == n - 1))

            @pl.when((early_prev > 0) & (sooner | usual))
            def _():
                take_early(jnp.where(sooner, jnp.where(me == 0, n - 1, 0), c))

            def end_piece(q):
                right(c, q).wait_recv()
                compute(c, span_of(q), False)

            @pl.when(go)
            def _():
                by_piece(p, end_piece)

            @pl.when(go & (p == pieces - 1) & ((i < (n - 1) * pieces - 1) | (me > 0)))
            def _():
                take_last(c)

            @pl.when((p == pieces - 1) & (me == 0) & (d < n - 1))
            def _():
                attend(d)

        @pl.when(me > 0)
        def _():
            if hold:
                attend_range(0, n - 2)
                for p in range(pieces - HELD, pieces - 1):
                    @pl.when(p >= early_prev)
                    def _():
                        right(n - 2, p).wait_recv()
                        compute(n - 2, span_of(p), False)

                take_last(n - 2)
            for t in range(max(n - 2, 0), n):
                attend(t)

        @pl.when(me == 0)
        def _():
            take_last(n - 1)
            attend(n - 1)


def in_hbm(a):
    return pltpu.with_memory_space_constraint(a, pltpu.HBM)


def per_device(stash, slot, doc_ids, norm_gain, w_query, w_key, value_weight):
    n, ns = lax.axis_size("tp"), lax.axis_size("section")
    _, slots, rows, width = stash.shape
    total = n * rows
    nq, nk = w_query.shape[1], w_key.shape[1]
    total_n = nq + nk + value_weight.shape[1]
    table = rope_tables(total)
    lanes = -(-rows // 128) * 128
    bf, f32, dma = jnp.bfloat16, jnp.float32, pltpu.SemaphoreType.DMA
    heads, stacked = nk // HEAD_SIZE, nq // nk * rows
    operands = (stash, doc_ids, norm_gain, jnp.asarray(table), w_query, w_key, value_weight)
    return pl.pallas_call(
        functools.partial(kernel, n, ns),
        out_shape=jax.ShapeDtypeStruct((1, total, nq), bf),
        in_specs=[pl.BlockSpec(memory_space=pltpu.SMEM)] + [ANY] * 7,
        out_specs=VMEM,
        scratch_shapes=[
            pltpu.VMEM((slots, rows, width), bf),
            pltpu.VMEM((SUBS, rows, width // SUBS), bf),
            pltpu.VMEM((8, lanes), jnp.int32),
            pltpu.VMEM((width, total_n), bf),
            pltpu.VMEM((n, SUBS, rows, width // SUBS), bf),
            pltpu.VMEM((n, EDGES[-2], rows, width // SUBS), bf),
            pltpu.VMEM((n, 8, lanes), jnp.int32),
            pltpu.VMEM((n, rows, total_n), f32),
            pltpu.VMEM((total, nq), bf),
            pltpu.VMEM((total, nk), bf),
            pltpu.VMEM((total, nk), bf),
            pltpu.VMEM((total, lanes), f32),
            pltpu.VMEM((n, 8, lanes), jnp.int32),
            pltpu.VMEM((heads, stacked, total), f32),
            pltpu.VMEM((heads, stacked, total), bf),
            dma,
            dma((max(n, rows // CHUNK),)),
            dma,
            dma((n, PIECES)),
            dma((n,)),
            dma,
            dma((n, PIECES - 1)),
            dma,
            dma,
            dma((n,)),
            dma,
            pltpu.SemaphoreType.REGULAR,
            pltpu.VMEM(doc_ids.shape, jnp.int32),
            pltpu.VMEM(norm_gain.shape, bf),
            pltpu.VMEM(table.shape, f32),
        ],
        compiler_params=pltpu.CompilerParams(
            collective_id=0, has_side_effects=True, vmem_limit_bytes=VMEM_GRANT
        ),
        cost_estimate=pl.CostEstimate(
            flops=2 * total * width * total_n, bytes_accessed=width * total_n * 2, transcendentals=0
        ),
    )(slot, *(in_hbm(a) for a in operands))


def solution(mesh):
    placed = (
        P("section", None, "tp", None),
        P("section"),
        P("section", None, "tp"),
        P(),
        P(None, "tp"),
        P(None, "tp"),
        P(None, "tp"),
    )
    return jax.shard_map(
        per_device, mesh=mesh, in_specs=placed, out_specs=P("section", None, "tp"), check_vma=False
    )
```
